512 devices in a mesh: chan: 128 (over z, y_hi, x), section: 4 (over y_lo, core).
Axes of the slice: x: 4, y: 8 (y_hi: 4, y_lo: 2; y = y_hi * 2 + y_lo), z: 8, core: 2. Of those that a mesh axis runs over, the one named last changes fastest.
Arguments:
- voltages: bfloat16 [2, 2, 36, 256, 188, 128], P(None, None, 'section', 'chan'), may hold values from -32 to 32
- weights: bfloat16 [2, 36, 256, 36, 188], P(None, 'section', 'chan'), may hold values from -4 to 4
- sat_index: int32 [2, 128, 2], P(None, 'chan'), may hold values from 0 to 63, as said below
- offsets: int32 [2, 128], replicated, may hold values from 0 to 127
- angles: float32 [64, 188], replicated, may hold values from -3 to 3
Outputs:
- visibilities: float32 [2, 36, 256, 1296], P(None, 'section', 'chan')
- new_weights: bfloat16 [2, 36, 256, 36, 188], P(None, 'section', 'chan')
The draws below stay inside these ranges and needn't reach their ends.
Inputs may be any that keep to these rules, and one draw needn't show every extreme that they name: `sat_index`: catalogue rows of the satellites nulled in each cycle and block of 2 channels.
All inputs are finite; a program needn't handle non-finite values.
Results may differ from the reference program's by a relative error of at most 0.0065.
Values may be sent and summed in bfloat16 or wider, within the bound.
A program may use at most 128 MiB of HBM per device.

```python
import math
import jax
import jax.numpy as jnp
from jax import lax

DISHES = 36
PORTS = 188
BEAMS = 36
TIME = 128
TS = 128
CYCLES = 2
NSAT = 2
K_DIR = 64
BLOCK_CH = 2
CHANNELS = 256
BLOCKS = 128


def catalogue(key):
    phases = jax.random.uniform(jax.random.fold_in(key, 11), (K_DIR, PORTS), jnp.float32, -3.0, 3.0)
    listed = jax.random.randint(jax.random.fold_in(key, 12), (CYCLES, BLOCKS, NSAT), 0, K_DIR, dtype=jnp.int32)
    return (phases, listed)


def draw_angles(key, part):
    return catalogue(key)[0]


def draw_sat_index(key, part):
    return catalogue(key)[1]


def draw_weights(key, part):
    phases, listed = catalogue(key)
    per_channel = jnp.repeat(listed, BLOCK_CH, axis=1)
    present = jnp.moveaxis(per_channel, 0, 1).reshape(CHANNELS, CYCLES * NSAT)
    cosine = jnp.cos(phases)[present]
    sine_part = jnp.sin(phases)[present]
    coeff_shape = (2, DISHES, CHANNELS, BEAMS, CYCLES * NSAT)
    noise_shape = (2, DISHES, CHANNELS, BEAMS, PORTS)
    spread = 0.5 / math.sqrt(PORTS)
    base = 1.0 / math.sqrt(2 * PORTS)
    coeff = jax.random.truncated_normal(jax.random.fold_in(key, 31), -4.0, 4.0, coeff_shape, jnp.float32) * spread
    noise_part = jax.random.truncated_normal(jax.random.fold_in(key, 32), -4.0, 4.0, noise_shape, jnp.float32) * base
    real_part = jnp.einsum('dfbk,fkp->dfbp', coeff[0], cosine) - jnp.einsum('dfbk,fkp->dfbp', coeff[1], sine_part)
    imag_part = jnp.einsum('dfbk,fkp->dfbp', coeff[0], sine_part) + jnp.einsum('dfbk,fkp->dfbp', coeff[1], cosine)
    return (noise_part + jnp.stack([real_part, imag_part])).astype(jnp.bfloat16)


def draw_voltages(key, part):
    phases, listed = catalogue(key)
    per_channel = jnp.repeat(listed, BLOCK_CH, axis=1)
    earlier = jnp.concatenate([per_channel[:1], per_channel[:-1]], axis=0)
    present = jnp.concatenate([per_channel, earlier], axis=2)
    cosine = jnp.cos(phases)[present]
    sine_part = jnp.sin(phases)[present]
    later = jnp.broadcast_to((jnp.arange(CYCLES) > 0).astype(jnp.float32)[:, None], (CYCLES, NSAT))
    active = jnp.concatenate([jnp.ones((CYCLES, NSAT), jnp.float32), later], axis=1)[:, None, :]
    full_shape = (CYCLES, 2, DISHES, CHANNELS, PORTS, TIME)
    noise_part = jax.random.truncated_normal(jax.random.fold_in(key, 21), -4.0, 4.0, full_shape, jnp.float32)
    strength = jnp.exp(jax.random.uniform(jax.random.fold_in(key, 22), (CYCLES, CHANNELS, 2 * NSAT), jnp.float32, math.log(0.03), math.log(0.12)))
    strength = strength * active
    signal = jax.random.truncated_normal(jax.random.fold_in(key, 23), -4.0, 4.0, (CYCLES, 2, DISHES, CHANNELS, 2 * NSAT, TIME), jnp.float32)
    gain_real = strength[..., None] * cosine
    gain_imag = strength[..., None] * sine_part
    real_part = jnp.einsum('cfsp,cdfst->cdfpt', gain_real, signal[:, 0]) - jnp.einsum('cfsp,cdfst->cdfpt', gain_imag, signal[:, 1])
    imag_part = jnp.einsum('cfsp,cdfst->cdfpt', gain_real, signal[:, 1]) + jnp.einsum('cfsp,cdfst->cdfpt', gain_imag, signal[:, 0])
    return (noise_part + jnp.stack([real_part, imag_part], axis=1)).astype(jnp.bfloat16)


def with_ends(array, own_key, low, high):
    longest = array.shape.index(max(array.shape))
    spots = []
    for shift in (0, 1):
        where = [jax.random.randint(jax.random.fold_in(own_key, axis), (), 0, length) for axis, length in enumerate(array.shape)]
        where[longest] = (where[longest] + shift) % array.shape[longest]
        spots.append(tuple(where))
    return array.at[spots[0]].set(low).at[spots[1]].set(high)


def setup_inputs(seed: int = 0) -> dict:
    key_of = jax.random.split(jax.random.key(seed), 6)
    return {
        "voltages": draw_voltages(jax.random.fold_in(key_of[5], 71), 0),
        "weights": draw_weights(jax.random.fold_in(key_of[5], 71), 0),
        "sat_index": draw_sat_index(jax.random.fold_in(key_of[5], 71), 0),
        "offsets": with_ends(jax.random.randint(key_of[3], (CYCLES, TS), 0, TIME), jax.random.fold_in(key_of[3], 1), 0, TIME - 1).astype(jnp.int32),
        "angles": draw_angles(jax.random.fold_in(key_of[5], 71), 0),
    }


LOADING = 100.0
HIGHEST = lax.Precision.HIGHEST


def complex_sums(left_side, right_side, pattern):
    left_wide = left_side.astype(jnp.float32)
    right_wide = right_side.astype(jnp.float32)
    turned = jnp.stack([left_wide[1], -left_wide[0]])
    real_part = jnp.einsum(pattern, left_wide, right_wide, precision=HIGHEST)
    imag_part = jnp.einsum(pattern, turned, right_wide, precision=HIGHEST)
    return jnp.stack([real_part, imag_part])


def beamform(weight, voltage_now):
    weight_wide = weight.astype(jnp.float32)
    voltage_wide = voltage_now.astype(jnp.float32)
    turned = jnp.stack([-weight_wide[1], weight_wide[0]])
    real_part = jnp.einsum('cdfbp,cdfpt->dfbt', weight_wide, voltage_wide, precision=HIGHEST)
    imag_part = jnp.einsum('cdfbp,cdfpt->dfbt', turned, voltage_wide, precision=HIGHEST)
    return jnp.stack([real_part, imag_part]).astype(jnp.bfloat16)


def null_update(weight, smooth, steer_real, steer_imag):
    real_weight = weight[0].astype(jnp.float32)
    imag_weight = weight[1].astype(jnp.float32)
    for slot_index in range(steer_real.shape[1]):
        along_real = steer_real[:, slot_index]
        along_imag = steer_imag[:, slot_index]
        null_real = (jnp.einsum('dfpq,fq->dfp', smooth[0], along_real, precision=HIGHEST)
                     - jnp.einsum('dfpq,fq->dfp', smooth[1], along_imag, precision=HIGHEST)
                     + LOADING * along_real)
        null_imag = (jnp.einsum('dfpq,fq->dfp', smooth[0], along_imag, precision=HIGHEST)
                     + jnp.einsum('dfpq,fq->dfp', smooth[1], along_real, precision=HIGHEST)
                     + LOADING * along_imag)
        inverse = 1.0 / jnp.sum(null_real * null_real + null_imag * null_imag, axis=-1)
        coeff_real = (jnp.einsum('dfp,dfbp->dfb', null_real, real_weight, precision=HIGHEST)
                      + jnp.einsum('dfp,dfbp->dfb', null_imag, imag_weight, precision=HIGHEST)) * inverse[..., None]
        coeff_imag = (jnp.einsum('dfp,dfbp->dfb', null_real, imag_weight, precision=HIGHEST)
                      - jnp.einsum('dfp,dfbp->dfb', null_imag, real_weight, precision=HIGHEST)) * inverse[..., None]
        wide_real = null_real[:, :, None, :]
        wide_imag = null_imag[:, :, None, :]
        real_weight = real_weight - (wide_real * coeff_real[..., None] - wide_imag * coeff_imag[..., None])
        imag_weight = imag_weight - (wide_real * coeff_imag[..., None] + wide_imag * coeff_real[..., None])
    return jnp.stack([real_weight, imag_weight]).astype(jnp.bfloat16)


def correlate(beam_out):
    def single_beam(beam_piece):
        return complex_sums(beam_piece, beam_piece, 'cdft,ceft->fde')

    result_sums = lax.map(single_beam, jnp.moveaxis(beam_out, 3, 0))
    return jnp.moveaxis(result_sums, 0, 1)


def reference(voltages, weights, sat_index, offsets, angles):
    cosine_table = jnp.cos(angles)
    sine_table = jnp.sin(angles)
    current = weights
    visibility = jnp.zeros((2, BEAMS, CHANNELS, DISHES, DISHES), jnp.float32)
    for cycle_index in range(CYCLES):
        listed = jnp.repeat(sat_index[cycle_index], BLOCK_CH, axis=0)
        steer_real = cosine_table[listed]
        steer_imag = sine_table[listed]
        pick_times = offsets[cycle_index]

        def each_dish(dish_items):
            voltage_one = dish_items[0][:, None]
            weight_one = dish_items[1][:, None]
            beam_out = beamform(weight_one, voltage_one)
            sampled = jnp.take(voltage_one, pick_times, axis=4)
            covariance = complex_sums(sampled, sampled, 'cdfpt,cdfqt->dfpq')
            padded = jnp.pad(covariance, ((0, 0), (0, 0), (1, 1), (0, 0), (0, 0)))
            smooth = padded[:, :, :-2] + padded[:, :, 1:-1] + padded[:, :, 2:]
            next_weights = null_update(weight_one, smooth, steer_real, steer_imag)
            return beam_out[:, 0], next_weights[:, 0]

        beam_out, next_weights = lax.map(
            each_dish, (jnp.moveaxis(voltages[cycle_index], 1, 0), jnp.moveaxis(current, 1, 0)))
        beam_out = jnp.moveaxis(beam_out, 0, 1)
        current = jnp.moveaxis(next_weights, 0, 1)
        visibility = visibility + correlate(beam_out)
    visibility = visibility * (1.0 / (CYCLES * TIME))
    return visibility.reshape(2, BEAMS, CHANNELS, DISHES * DISHES), current
```

```python
import functools

import jax
import jax.numpy as jnp
from jax import lax
from jax.experimental import pallas as pl
from jax.experimental.pallas import tpu as pltpu
from jax.sharding import PartitionSpec as P

LOADING = 100.0
MESH = pl.DeviceIdType.MESH
F32 = jnp.float32
BF16 = jnp.bfloat16
CYC, DISH, CH, BEAM, PORT, TIME = 2, 9, 2, 36, 188, 128
SEC = 4
ROWS = CH * PORT
LANES = 384
TILES = LANES // TIME
WR = BEAM * CH
PER = WR // SEC
BLK = DISH * PER
BLKP = 168
ALL = SEC * DISH
ALLP = 40


def dot(a, b):
    return lax.dot_general(a, b, (((1,), (0,)), ((), ())), preferred_element_type=F32)


def dot_t(a, b):
    return lax.dot_general(a, b, (((1,), (1,)), ((), ())), preferred_element_type=F32)


def iota(shape, dim):
    return lax.broadcasted_iota(jnp.int32, shape, dim)


def even_lanes(shape):
    return (iota(shape, 1) & 1) == 0


def split(x):
    high = x.astype(BF16)
    return high, (x - high.astype(F32)).astype(BF16)


def strided(ref, rows):
    return jnp.concatenate([ref[k, rows, :] for k in range(TILES)], axis=1)


def lane_up(x):
    return pltpu.roll(x, 1, 1)


def lane_down(x):
    return pltpu.roll(x, LANES - 1, 1)


def kernel(
    chans,
    volt, w_in, sat_in, offs, table,
    vis, w_out,
    x, we, sat_l, sat_r, steer, vv, packed, halo_l, halo_r, ana, syn, nul, stage, sbuf, recv, wide, corr,
    x_sem, sat_ssem, sat_rsem, halo_ssem, halo_rsem, beam_ssem, beam_rsem,
):
    me = lax.axis_index("chan")
    sec = lax.axis_index("section")
    left = lax.rem(me + chans - 1, chans)
    right = lax.rem(me + 1, chans)

    def load(c, d, z):
        return pltpu.make_async_copy(
            volt.at[c, z, d],
            x.at[c, d, pl.ds(0, ROWS), pl.ds(z * TIME, TIME)],
            x_sem.at[c, d, z],
        )

    for c in range(CYC):
        for d in range(DISH):
            for z in range(2):
                load(c, d, z).start()

    barrier = pltpu.get_barrier_semaphore()
    for j in range(1, SEC):
        pl.semaphore_signal(
            barrier, inc=1, device_id={"section": lax.rem(sec + j, SEC)}, device_id_type=MESH
        )
    for peer in (left, right):
        pl.semaphore_signal(barrier, inc=1, device_id={"chan": peer}, device_id_type=MESH)
    pl.semaphore_wait(barrier, SEC + 1)

    def sat_copy(side):
        return pltpu.make_async_remote_copy(
            src_ref=sat_in,
            dst_ref=sat_r if side == 0 else sat_l,
            send_sem=sat_ssem.at[side],
            recv_sem=sat_rsem.at[side],
            device_id={"chan": left if side == 0 else right},
            device_id_type=MESH,
        )

    for side in range(2):
        sat_copy(side).start()

    spread = (lax.shift_right_logical(iota((PORT, LANES), 1), 1) == iota((PORT, LANES), 0)).astype(
        F32
    ).astype(BF16)
    own = (iota((WR, LANES), 0) & 1) == (iota((WR, LANES), 1) & 1)
    for c in range(CYC):
        for d in range(DISH):
            x[c, d, pl.ds(ROWS, LANES - ROWS), :] = jnp.zeros((LANES - ROWS, 2 * TIME), BF16)
    wide[:, pl.ds(ALL * PER, (ALLP - ALL) * PER), :] = jnp.zeros(
        (2 * CYC, (ALLP - ALL) * PER, TIME), F32
    )
    for d in range(DISH):
        for z in range(2):
            grown = dot(w_in[z, d], spread)
            we[d, pl.ds(z * WR, WR), :] = jnp.where(own, grown, 0.0).astype(BF16)

    def beams(c):
        for d in range(DISH):
            if c == 0:
                load(c, d, 0).wait()
                load(c, d, 1).wait()
            both = dot(we[d], x[c, d])
            real = both[:WR, :TIME] + both[WR:, TIME:]
            imag = both[:WR, TIME:] - both[WR:, :TIME]
            for s in range(SEC):
                rows = pl.ds(d * PER, PER)
                stage[s, rows, pl.ds(0, TIME)] = real[s * PER : (s + 1) * PER]
                stage[s, rows, pl.ds(TIME, TIME)] = imag[s * PER : (s + 1) * PER]
        for s in range(SEC):
            sbuf[c, s] = stage[s].astype(BF16)

    def beam_copy(c, j):
        peer = lax.rem(sec + j, SEC)
        return pltpu.make_async_remote_copy(
            src_ref=sbuf.at[c, peer],
            dst_ref=recv.at[c, sec],
            send_sem=beam_ssem.at[c, j - 1],
            recv_sem=beam_rsem.at[c, j - 1],
            device_id={"section": peer},
            device_id_type=MESH,
        )

    def send_beams(c):
        for j in (2, 3, 1):
            beam_copy(c, j).start()
        recv[c, sec] = sbuf[c, sec]

    beams(0)
    send_beams(0)

    grown_table = []
    for z in range(2):
        for part in split(table[z]):
            grown_table.append(dot(part, spread).astype(BF16))
    for side in range(2):
        sat_copy(side).wait()
    row = iota((8, TIME), 0)
    keep = (iota((8, LANES), 0) >= 4) == ((iota((8, LANES), 1) & 1) == 1)
    for c in range(CYC):
        index = jnp.where(
            (row & 3) < 2, sat_in[c], jnp.where(row < 4, sat_l[c], sat_r[c])
        )
        hot = (index == iota((8, TIME), 1)).astype(F32).astype(BF16)[:, :64]
        parts = [dot(hot, part) for part in grown_table]
        for i, (h, l) in enumerate(((0, 1), (2, 3))):
            steer[c, i] = parts[h] + parts[l]
        stacked = [jnp.where(keep, parts[i], 0.0) for i in (0, 2, 1, 3)]
        for i in range(4):
            ana[c, pl.ds(8 * i, 8), :] = stacked[i]

    even4 = even_lanes((4, LANES))

    def null_vectors(c):
        times = (offs[pl.ds(c, 1), :] == iota((TIME, TIME), 0)).astype(F32).astype(BF16)
        count = dot_t(jnp.ones((8, TIME), BF16), times)
        probe = ana[c].astype(BF16)
        for d in range(DISH):
            if c == 1:
                load(c, d, 0).wait()
                load(c, d, 1).wait()
            block = x[c, d]
            out = dot(probe, block)
            out = out[:16] + out[16:]
            y_real = (out[:8, :TIME] + out[8:, TIME:]) * count
            y_imag = (out[8:, :TIME] - out[:8, TIME:]) * count
            lines = jnp.concatenate(
                [
                    jnp.concatenate([y_real, -y_imag], axis=1),
                    jnp.concatenate([y_imag, y_real], axis=1),
                ],
                axis=0,
            )
            high, low = split(lines)
            back = dot_t(high, block) + dot_t(low, block)
            for i in range(2):
                kept = jnp.where(even4, back[8 * i : 8 * i + 4], back[8 * i + 4 : 8 * i + 8])
                for k in range(TILES):
                    vv[c, k, pl.ds(8 * d + 4 * i, 4), :] = kept[:, k * TIME : (k + 1) * TIME]

    even = even_lanes((DISH, LANES))

    def halo_copy(c, side):
        return pltpu.make_async_remote_copy(
            src_ref=packed.at[c, side],
            dst_ref=(halo_r if side == 0 else halo_l).at[c],
            send_sem=halo_ssem.at[c, side],
            recv_sem=halo_rsem.at[c, side],
            device_id={"chan": left if side == 0 else right},
            device_id_type=MESH,
        )

    def take(c, q):
        return strided(vv.at[c], pl.ds(q, DISH, stride=8))

    def send_halo(c):
        for i in range(2):
            first, second = take(c, 4 * i + 2), take(c, 4 * i + 3)
            packed[c, 0, i, pl.ds(0, DISH), :] = jnp.where(even, first, lane_up(second))
            packed[c, 1, i, pl.ds(0, DISH), :] = jnp.where(even, lane_down(first), second)
        for side in range(2):
            halo_copy(c, side).start()

    packed[...] = jnp.zeros_like(packed)
    null_vectors(0)
    send_halo(0)
    null_vectors(1)
    send_halo(1)

    def lane_sum(v):
        e = jnp.sum(jnp.where(even, v, 0.0), axis=1, keepdims=True)
        o = jnp.sum(jnp.where(even, 0.0, v), axis=1, keepdims=True)
        return jnp.where(even, e, o)

    def project_vectors(c):
        for side in range(2):
            halo_copy(c, side).wait()
        u = []
        for i in range(2):
            from_l = jnp.where(me == 0, 0.0, halo_l[c, i, pl.ds(0, DISH), :])
            from_r = jnp.where(me == chans - 1, 0.0, halo_r[c, i, pl.ds(0, DISH), :])
            halo = (
                jnp.where(even, from_l, lane_up(from_r)),
                jnp.where(even, lane_down(from_l), from_r),
            )
            for s in range(2):
                v = take(c, 4 * i + s)
                v = v + jnp.where(even, lane_down(v), lane_up(v))
                u.append(v + halo[s] + LOADING * steer[c, i, pl.ds(s, 1), :])
        u0r, u1r, u0i, u1i = u
        inv0 = 1.0 / lane_sum(u0r * u0r + u0i * u0i)
        inv1 = 1.0 / lane_sum(u1r * u1r + u1i * u1i)
        t0r, t0i = u0r * inv0, u0i * inv0
        kr = lane_sum(t0r * u1r + t0i * u1i)
        ki = lane_sum(t0r * u1i - t0i * u1r)
        t1r = (u1r - (u0r * kr - u0i * ki)) * inv1
        t1i = (u1i - (u0r * ki + u0i * kr)) * inv1
        for q, (t, v) in enumerate(((t0r, u0r), (t0i, u0i), (t1r, u1r), (t1i, u1i))):
            for k in range(TILES):
                syn[k, pl.ds(16 * q, DISH), :] = t[:, k * TIME : (k + 1) * TIME]
            nul[pl.ds(16 * q, DISH), :] = v

    def project(d):
        high, low = split(strided(syn, pl.ds(d, 4, stride=16)))
        old = we[d]
        g = dot_t(old, high) + dot_t(old, low)
        gr, gi = g[:WR], g[WR:]
        v = [nul[pl.ds(16 * q + d, 1), :] for q in range(4)]
        new_r = old[:WR].astype(F32)
        new_i = old[WR:].astype(F32)
        for s in range(2):
            cr = gr[:, 2 * s : 2 * s + 1] + gi[:, 2 * s + 1 : 2 * s + 2]
            ci = gi[:, 2 * s : 2 * s + 1] - gr[:, 2 * s + 1 : 2 * s + 2]
            vr, vi = v[2 * s], v[2 * s + 1]
            new_r = new_r - (vr * cr - vi * ci)
            new_i = new_i - (vr * ci + vi * cr)
        we[d, pl.ds(0, WR), :] = jnp.where(own, new_r, 0.0).astype(BF16)
        we[d, pl.ds(WR, WR), :] = jnp.where(own, new_i, 0.0).astype(BF16)

    project_vectors(0)
    for d in range(DISH):
        project(d)
    beams(1)
    send_beams(1)

    project_vectors(1)
    gather = (lax.shift_right_logical(iota((LANES, PORT), 0), 1) == iota((LANES, PORT), 1)).astype(
        F32
    ).astype(BF16)
    for d in range(DISH):
        project(d)
    for d in range(DISH):
        for z in range(2):
            w_out[z, d] = dot(we[d, pl.ds(z * WR, WR), :], gather).astype(BF16)

    for c in range(CYC):
        for j in range(1, SEC):
            beam_copy(c, j).wait_recv()
        for s in range(SEC):
            block = recv[c, s].astype(F32)[:BLK]
            for z in range(2):
                wide[2 * c + z, pl.ds(s * BLK, BLK), :] = block[:, z * TIME : (z + 1) * TIME]

    for r in range(PER):
        lanes = [wide[k, pl.ds(r, ALLP, stride=PER), :] for k in range(2 * CYC)]
        straight = jnp.concatenate(lanes, axis=1)
        turned = jnp.concatenate([lanes[1], -lanes[0], lanes[3], -lanes[2]], axis=1)
        right_side = straight.astype(BF16)
        result = dot_t(jnp.concatenate([straight, turned], axis=0).astype(BF16), right_side)
        result = result * (1.0 / (CYC * TIME))
        for z in range(2):
            corr[z, pl.ds(r * ALLP, ALLP), pl.ds(0, ALLP)] = result[z * ALLP : (z + 1) * ALLP]
    for z in range(2):
        for d in range(ALL):
            vis[z, :, pl.ds(d * ALL, ALL)] = corr[z, pl.ds(d, PER, stride=ALLP), :][:, :ALL]

    for c in range(CYC):
        for j in range(1, SEC):
            beam_copy(c, j).wait_send()


def per_device(chans, voltages, weights, sat_index, offsets, angles):
    volt = voltages.transpose(0, 1, 2, 4, 3, 5).reshape(CYC, 2, DISH, ROWS, TIME)
    w_in = weights.transpose(0, 1, 3, 2, 4).reshape(2, DISH, WR, PORT)
    sat = jnp.broadcast_to(sat_index.reshape(CYC, 1, 2, 1), (CYC, 4, 2, TIME)).reshape(CYC, 8, TIME)
    table = jnp.stack([jnp.cos(angles), jnp.sin(angles)])
    vmem = pl.BlockSpec(memory_space=pltpu.VMEM)
    dma = pltpu.SemaphoreType.DMA
    vis, new = pl.pallas_call(
        functools.partial(kernel, chans),
        out_shape=(
            jax.ShapeDtypeStruct((2, PER, ALL * ALL), F32),
            jax.ShapeDtypeStruct((2, DISH, WR, PORT), BF16),
        ),
        in_specs=[pl.BlockSpec(memory_space=pl.ANY), vmem, vmem, vmem, vmem],
        out_specs=(vmem, vmem),
        scratch_shapes=[
            pltpu.VMEM((CYC, DISH, LANES, 2 * TIME), BF16),
            pltpu.VMEM((DISH, 2 * WR, LANES), BF16),
            pltpu.VMEM((CYC, 8, TIME), jnp.int32),
            pltpu.VMEM((CYC, 8, TIME), jnp.int32),
            pltpu.VMEM((CYC, 2, 8, LANES), F32),
            pltpu.VMEM((CYC, TILES, DISH * 8, TIME), F32),
            pltpu.VMEM((CYC, 2, 2, 16, LANES), F32),
            pltpu.VMEM((CYC, 2, 16, LANES), F32),
            pltpu.VMEM((CYC, 2, 16, LANES), F32),
            pltpu.VMEM((CYC, 32, LANES), F32),
            pltpu.VMEM((TILES, 64, TIME), F32),
            pltpu.VMEM((64, LANES), F32),
            pltpu.VMEM((SEC, BLKP, 2 * TIME), F32),
            pltpu.VMEM((CYC, SEC, BLKP, 2 * TIME), BF16),
            pltpu.VMEM((CYC, SEC, BLKP, 2 * TIME), BF16),
            pltpu.VMEM((2 * CYC, ALLP * PER, TIME), F32),
            pltpu.VMEM((2, PER * ALLP, TIME), F32),
            dma((CYC, DISH, 2)),
            dma((2,)),
            dma((2,)),
            dma((CYC, 2)),
            dma((CYC, 2)),
            dma((CYC, SEC - 1)),
            dma((CYC, SEC - 1)),
        ],
        compiler_params=pltpu.CompilerParams(collective_id=0, has_side_effects=True),
    )(volt, w_in, sat, offsets, table)
    visibility = vis.reshape(2, DISH, CH, ALL * ALL)
    new = new.reshape(2, DISH, BEAM, CH, PORT).transpose(0, 1, 3, 2, 4)
    return visibility, new


def solution(mesh):
    placed = (
        P(None, None, "section", "chan", None, None),
        P(None, "section", "chan", None, None),
        P(None, "chan", None),
        P(),
        P(),
    )
    return jax.shard_map(
        functools.partial(per_device, mesh.shape["chan"]),
        mesh=mesh,
        in_specs=placed,
        out_specs=(P(None, "section", "chan", None), P(None, "section", "chan", None, None)),
        check_vma=False,
    )
```

```python
import functools

import jax
import jax.numpy as jnp
from jax import lax
from jax.experimental import pallas as pl
from jax.experimental.pallas import tpu as pltpu
from jax.sharding import PartitionSpec as P

LOADING = 100.0
MESH = pl.DeviceIdType.MESH
F32 = jnp.float32
BF16 = jnp.bfloat16
CYC, DISH, CH, BEAM, PORT, TIME = 2, 9, 2, 36, 188, 128
SEC = 4
ROWS = CH * PORT
LANES = 384
TILES = LANES // TIME
WR = BEAM * CH
PER = WR // SEC
BLK = DISH * PER
BLKP = 168
ALL = SEC * DISH
ALLP = 40


def dot(a, b):
    return lax.dot_general(a, b, (((1,), (0,)), ((), ())), preferred_element_type=F32)


def dot_t(a, b):
    return lax.dot_general(a, b, (((1,), (1,)), ((), ())), preferred_element_type=F32)


def iota(shape, dim):
    return lax.broadcasted_iota(jnp.int32, shape, dim)


def even_lanes(shape):
    return (iota(shape, 1) & 1) == 0


def split(x):
    high = x.astype(BF16)
    return high, (x - high.astype(F32)).astype(BF16)


def strided(ref, rows):
    return jnp.concatenate([ref[k, rows, :] for k in range(TILES)], axis=1)


def lane_up(x):
    return pltpu.roll(x, 1, 1)


def lane_down(x):
    return pltpu.roll(x, LANES - 1, 1)


def kernel(
    chans,
    volt, w_hbm, sat_hbm, offs_hbm, ang_hbm,
    vis, w_out,
    x, w_in, sat_in, offs, ang, flat, we, sat_l, sat_r, steer, vv, packed, halo_l, halo_r, ana, syn, nul, stage, sbuf, recv, wide, corr,
    in_sem, x_sem, sat_ssem, sat_rsem, halo_ssem, halo_rsem, beam_ssem, beam_rsem,
):
    me = lax.axis_index("chan")
    sec = lax.axis_index("section")
    left = lax.rem(me + chans - 1, chans)
    right = lax.rem(me + 1, chans)

    def load(c, d, z):
        return pltpu.make_async_copy(
            volt.at[c, z, d],
            x.at[c, d, pl.ds(0, ROWS), pl.ds(z * TIME, TIME)],
            x_sem.at[c, d, z],
        )

    sat_l[...] = jnp.zeros_like(sat_l)
    sat_r[...] = jnp.zeros_like(sat_r)
    halo_l[...] = jnp.zeros_like(halo_l)
    halo_r[...] = jnp.zeros_like(halo_r)

    barrier = pltpu.get_barrier_semaphore()
    for j in range(1, SEC):
        pl.semaphore_signal(
            barrier, inc=1, device_id={"section": lax.rem(sec + j, SEC)}, device_id_type=MESH
        )
    sides = ((me > 0, left), (me < chans - 1, right))
    for exists, peer in sides:

        @pl.when(exists)
        def _():
            pl.semaphore_signal(barrier, inc=1, device_id={"chan": peer}, device_id_type=MESH)

    small = [
        pltpu.make_async_copy(source, target, in_sem.at[i])
        for i, (source, target) in enumerate(
            ((ang_hbm, ang), (w_hbm, w_in), (sat_hbm, sat_in), (offs_hbm, offs))
        )
    ]
    for copy in small:
        copy.start()
    for c in range(CYC):
        for d in range(DISH):
            for z in range(2):
                load(c, d, z).start()

    def sat_copy(side):
        return pltpu.make_async_remote_copy(
            src_ref=sat_in,
            dst_ref=sat_r if side == 0 else sat_l,
            send_sem=sat_ssem.at[side],
            recv_sem=sat_rsem.at[side],
            device_id={"chan": left if side == 0 else right},
            device_id_type=MESH,
        )

    spread = (lax.shift_right_logical(iota((PORT, LANES), 1), 1) == iota((PORT, LANES), 0)).astype(
        F32
    ).astype(BF16)
    own = (iota((WR, LANES), 0) & 1) == (iota((WR, LANES), 1) & 1)
    for c in range(CYC):
        for d in range(DISH):
            x[c, d, pl.ds(ROWS, LANES - ROWS), :] = jnp.zeros((LANES - ROWS, 2 * TIME), BF16)
    wide[:, pl.ds(ALL * PER, (ALLP - ALL) * PER), :] = jnp.zeros(
        (2 * CYC, (ALLP - ALL) * PER, TIME), F32
    )
    small[0].wait()
    grown_table = []
    for values in (jnp.cos(ang[...]), jnp.sin(ang[...])):
        for part in split(values):
            grown_table.append(dot(part, spread).astype(BF16))
    small[1].wait()
    for d in range(DISH):
        for z in range(2):
            grown = dot(w_in[z, d].reshape(WR, PORT), spread)
            we[d, pl.ds(z * WR, WR), :] = jnp.where(own, grown, 0.0).astype(BF16)

    pl.semaphore_wait(barrier, SEC - 1 + sum(e.astype(jnp.int32) for e, _peer in sides))
    small[2].wait()
    small[3].wait()
    for side in range(2):

        @pl.when(sides[side][0])
        def _():
            sat_copy(side).start()

    def beams(c):
        for d in range(DISH):
            if c == 0:
                load(c, d, 0).wait()
                load(c, d, 1).wait()
            both = dot(we[d], x[c, d])
            real = both[:WR, :TIME] + both[WR:, TIME:]
            imag = both[:WR, TIME:] - both[WR:, :TIME]
            for s in range(SEC):
                rows = pl.ds(d * PER, PER)
                stage[s, rows, pl.ds(0, TIME)] = real[s * PER : (s + 1) * PER]
                stage[s, rows, pl.ds(TIME, TIME)] = imag[s * PER : (s + 1) * PER]
        for s in range(SEC):
            sbuf[c, s] = stage[s].astype(BF16)

    def beam_copy(c, j):
        peer = lax.rem(sec + j, SEC)
        return pltpu.make_async_remote_copy(
            src_ref=sbuf.at[c, peer],
            dst_ref=recv.at[c, sec],
            send_sem=beam_ssem.at[c, j - 1],
            recv_sem=beam_rsem.at[c, j - 1],
            device_id={"section": peer},
            device_id_type=MESH,
        )

    def send_beams(c):
        for j in (2, 3, 1):
            beam_copy(c, j).start()
        recv[c, sec] = sbuf[c, sec]

    beams(0)
    send_beams(0)

    for side in range(2):

        @pl.when(sides[1 - side][0])
        def _():
            sat_copy(side).wait_recv()

    row = iota((8, TIME), 0)
    keep = (iota((8, LANES), 0) >= 4) == ((iota((8, LANES), 1) & 1) == 1)
    for c in range(CYC):
        own_s, left_s, right_s = (
            jnp.where((row & 1) == 0, ref[pl.ds(c, 1), pl.ds(0, 1)], ref[pl.ds(c, 1), pl.ds(1, 1)])
            for ref in (sat_in, sat_l, sat_r)
        )
        index = jnp.where((row & 3) < 2, own_s, jnp.where(row < 4, left_s, right_s))
        hot = (index == iota((8, TIME), 1)).astype(F32).astype(BF16)[:, :64]
        parts = [dot(hot, part) for part in grown_table]
        for i, (h, l) in enumerate(((0, 1), (2, 3))):
            steer[c, i] = parts[h] + parts[l]
        stacked = [jnp.where(keep, parts[i], 0.0) for i in (0, 2, 1, 3)]
        for i in range(4):
            ana[c, pl.ds(8 * i, 8), :] = stacked[i]

    even4 = even_lanes((4, LANES))

    def null_vectors(c):
        times = (offs[pl.ds(c, 1), :] == iota((TIME, TIME), 0)).astype(F32).astype(BF16)
        count = dot_t(jnp.ones((8, TIME), BF16), times)
        probe = ana[c].astype(BF16)
        for d in range(DISH):
            if c == 1:
                load(c, d, 0).wait()
                load(c, d, 1).wait()
            block = x[c, d]
            out = dot(probe, block)
            out = out[:16] + out[16:]
            y_real = (out[:8, :TIME] + out[8:, TIME:]) * count
            y_imag = (out[8:, :TIME] - out[:8, TIME:]) * count
            lines = jnp.concatenate(
                [
                    jnp.concatenate([y_real, -y_imag], axis=1),
                    jnp.concatenate([y_imag, y_real], axis=1),
                ],
                axis=0,
            )
            high, low = split(lines)
            back = dot_t(high, block) + dot_t(low, block)
            for i in range(2):
                kept = jnp.where(even4, back[8 * i : 8 * i + 4], back[8 * i + 4 : 8 * i + 8])
                for k in range(TILES):
                    vv[c, k, pl.ds(8 * d + 4 * i, 4), :] = kept[:, k * TIME : (k + 1) * TIME]

    even = even_lanes((DISH, LANES))

    def halo_copy(c, side):
        return pltpu.make_async_remote_copy(
            src_ref=packed.at[c, side],
            dst_ref=(halo_r if side == 0 else halo_l).at[c],
            send_sem=halo_ssem.at[c, side],
            recv_sem=halo_rsem.at[c, side],
            device_id={"chan": left if side == 0 else right},
            device_id_type=MESH,
        )

    def take(c, q):
        return strided(vv.at[c], pl.ds(q, DISH, stride=8))

    def send_halo(c):
        for i in range(2):
            first, second = take(c, 4 * i + 2), take(c, 4 * i + 3)
            packed[c, 0, i, pl.ds(0, DISH), :] = jnp.where(even, first, lane_up(second))
            packed[c, 1, i, pl.ds(0, DISH), :] = jnp.where(even, lane_down(first), second)
        for side in range(2):

            @pl.when(sides[side][0])
            def _():
                halo_copy(c, side).start()

    packed[...] = jnp.zeros_like(packed)
    null_vectors(0)
    send_halo(0)
    null_vectors(1)
    send_halo(1)

    def lane_sum(v):
        e = jnp.sum(jnp.where(even, v, 0.0), axis=1, keepdims=True)
        o = jnp.sum(jnp.where(even, 0.0, v), axis=1, keepdims=True)
        return jnp.where(even, e, o)

    def project_vectors(c):
        for side in range(2):

            @pl.when(sides[1 - side][0])
            def _():
                halo_copy(c, side).wait_recv()

        u = []
        for i in range(2):
            from_l = halo_l[c, i, pl.ds(0, DISH), :]
            from_r = halo_r[c, i, pl.ds(0, DISH), :]
            halo = (
                jnp.where(even, from_l, lane_up(from_r)),
                jnp.where(even, lane_down(from_l), from_r),
            )
            for s in range(2):
                v = take(c, 4 * i + s)
                v = v + jnp.where(even, lane_down(v), lane_up(v))
                u.append(v + halo[s] + LOADING * steer[c, i, pl.ds(s, 1), :])
        u0r, u1r, u0i, u1i = u
        inv0 = 1.0 / lane_sum(u0r * u0r + u0i * u0i)
        inv1 = 1.0 / lane_sum(u1r * u1r + u1i * u1i)
        t0r, t0i = u0r * inv0, u0i * inv0
        kr = lane_sum(t0r * u1r + t0i * u1i)
        ki = lane_sum(t0r * u1i - t0i * u1r)
        t1r = (u1r - (u0r * kr - u0i * ki)) * inv1
        t1i = (u1i - (u0r * ki + u0i * kr)) * inv1
        for q, (t, v) in enumerate(((t0r, u0r), (t0i, u0i), (t1r, u1r), (t1i, u1i))):
            for k in range(TILES):
                syn[k, pl.ds(16 * q, DISH), :] = t[:, k * TIME : (k + 1) * TIME]
            nul[pl.ds(16 * q, DISH), :] = v

    def project(d):
        high, low = split(strided(syn, pl.ds(d, 4, stride=16)))
        old = we[d]
        g = dot_t(old, high) + dot_t(old, low)
        gr, gi = g[:WR], g[WR:]
        v = [nul[pl.ds(16 * q + d, 1), :] for q in range(4)]
        new_r = old[:WR].astype(F32)
        new_i = old[WR:].astype(F32)
        for s in range(2):
            cr = gr[:, 2 * s : 2 * s + 1] + gi[:, 2 * s + 1 : 2 * s + 2]
            ci = gi[:, 2 * s : 2 * s + 1] - gr[:, 2 * s + 1 : 2 * s + 2]
            vr, vi = v[2 * s], v[2 * s + 1]
            new_r = new_r - (vr * cr - vi * ci)
            new_i = new_i - (vr * ci + vi * cr)
        we[d, pl.ds(0, WR), :] = jnp.where(own, new_r, 0.0).astype(BF16)
        we[d, pl.ds(WR, WR), :] = jnp.where(own, new_i, 0.0).astype(BF16)

    project_vectors(0)
    for d in range(DISH):
        project(d)
    beams(1)
    send_beams(1)

    project_vectors(1)
    gather = (lax.shift_right_logical(iota((LANES, PORT), 0), 1) == iota((LANES, PORT), 1)).astype(
        F32
    ).astype(BF16)
    for d in range(DISH):
        project(d)
    for d in range(DISH):
        for z in range(2):
            dense = dot(we[d, pl.ds(z * WR, WR), :], gather).astype(BF16)
            w_out[z, d] = dense.reshape(BEAM, CH, PORT)

    for c in range(CYC):
        for j in range(1, SEC):
            beam_copy(c, j).wait_recv()
        for s in range(SEC):
            block = recv[c, s].astype(F32)[:BLK]
            for z in range(2):
                wide[2 * c + z, pl.ds(s * BLK, BLK), :] = block[:, z * TIME : (z + 1) * TIME]

    for r in range(PER):
        lanes = [wide[k, pl.ds(r, ALLP, stride=PER), :] for k in range(2 * CYC)]
        straight = jnp.concatenate(lanes, axis=1)
        turned = jnp.concatenate([lanes[1], -lanes[0], lanes[3], -lanes[2]], axis=1)
        right_side = straight.astype(BF16)
        result = dot_t(jnp.concatenate([straight, turned], axis=0).astype(BF16), right_side)
        result = result * (1.0 / (CYC * TIME))
        for z in range(2):
            corr[z, pl.ds(r * ALLP, ALLP), pl.ds(0, ALLP)] = result[z * ALLP : (z + 1) * ALLP]
    for z in range(2):
        for d in range(ALL):
            flat[z, :, pl.ds(d * ALL, ALL)] = corr[z, pl.ds(d, PER, stride=ALLP), :][:, :ALL]
        vis[z] = flat[z].reshape(DISH, CH, ALL * ALL)

    for c in range(CYC):
        for j in range(1, SEC):
            beam_copy(c, j).wait_send()
    for side in range(2):

        @pl.when(sides[side][0])
        def _():
            sat_copy(side).wait_send()
            for c in range(CYC):
                halo_copy(c, side).wait_send()


def per_device(chans, voltages, weights, sat_index, offsets, angles):
    volt = voltages.transpose(0, 1, 2, 4, 3, 5).reshape(CYC, 2, DISH, ROWS, TIME)
    w_in = weights.transpose(0, 1, 3, 2, 4)
    sat = sat_index.reshape(CYC, 2)
    vmem = pl.BlockSpec(memory_space=pltpu.VMEM)
    hbm = pl.BlockSpec(memory_space=pltpu.HBM)
    dma = pltpu.SemaphoreType.DMA
    vis, new = pl.pallas_call(
        functools.partial(kernel, chans),
        out_shape=(
            jax.ShapeDtypeStruct((2, DISH, CH, ALL * ALL), F32),
            jax.ShapeDtypeStruct((2, DISH, BEAM, CH, PORT), BF16),
        ),
        in_specs=[hbm] * 5,
        out_specs=(vmem, vmem),
        scratch_shapes=[
            pltpu.VMEM((CYC, DISH, LANES, 2 * TIME), BF16),
            pltpu.VMEM((2, DISH, BEAM, CH, PORT), BF16),
            pltpu.VMEM((CYC, 2), jnp.int32),
            pltpu.VMEM((CYC, TIME), jnp.int32),
            pltpu.VMEM((64, PORT), F32),
            pltpu.VMEM((2, PER, ALL * ALL), F32),
            pltpu.VMEM((DISH, 2 * WR, LANES), BF16),
            pltpu.VMEM((CYC, 2), jnp.int32),
            pltpu.VMEM((CYC, 2), jnp.int32),
            pltpu.VMEM((CYC, 2, 8, LANES), F32),
            pltpu.VMEM((CYC, TILES, DISH * 8, TIME), F32),
            pltpu.VMEM((CYC, 2, 2, 16, LANES), F32),
            pltpu.VMEM((CYC, 2, 16, LANES), F32),
            pltpu.VMEM((CYC, 2, 16, LANES), F32),
            pltpu.VMEM((CYC, 32, LANES), F32),
            pltpu.VMEM((TILES, 64, TIME), F32),
            pltpu.VMEM((64, LANES), F32),
            pltpu.VMEM((SEC, BLKP, 2 * TIME), F32),
            pltpu.VMEM((CYC, SEC, BLKP, 2 * TIME), BF16),
            pltpu.VMEM((CYC, SEC, BLKP, 2 * TIME), BF16),
            pltpu.VMEM((2 * CYC, ALLP * PER, TIME), F32),
            pltpu.VMEM((2, PER * ALLP, TIME), F32),
            dma((4,)),
            dma((CYC, DISH, 2)),
            dma((2,)),
            dma((2,)),
            dma((CYC, 2)),
            dma((CYC, 2)),
            dma((CYC, SEC - 1)),
            dma((CYC, SEC - 1)),
        ],
        compiler_params=pltpu.CompilerParams(
            collective_id=0, has_side_effects=True, vmem_limit_bytes=24 << 20
        ),
    )(*(pltpu.with_memory_space_constraint(a, pltpu.HBM) for a in (volt, w_in, sat, offsets, angles)))
    return vis, new.transpose(0, 1, 3, 2, 4)


def solution(mesh):
    placed = (
        P(None, None, "section", "chan", None, None),
        P(None, "section", "chan", None, None),
        P(None, "chan", None),
        P(),
        P(),
    )
    return jax.shard_map(
        functools.partial(per_device, mesh.shape["chan"]),
        mesh=mesh,
        in_specs=placed,
        out_specs=(P(None, "section", "chan", None), P(None, "section", "chan", None, None)),
        check_vma=False,
    )
```

```python
import functools

import jax
import jax.numpy as jnp
from jax import lax
from jax.experimental import pallas as pl
from jax.experimental.pallas import tpu as pltpu
from jax.sharding import PartitionSpec as P

LOADING = 100.0
MESH = pl.DeviceIdType.MESH
F32 = jnp.float32
BF16 = jnp.bfloat16
CYC, DISH, CH, BEAM, PORT, TIME = 2, 9, 2, 36, 188, 128
SEC = 4
ROWS = CH * PORT
LANES = 384
TILES = LANES // TIME
WR = BEAM * CH
PER = WR // SEC
PARTS = 3
PART = DISH // PARTS
BLK = PART * PER
BLKP = 56
ALL = SEC * DISH
ALLP = 40


def dot(a, b):
    return lax.dot_general(a, b, (((1,), (0,)), ((), ())), preferred_element_type=F32)


def dot_t(a, b):
    return lax.dot_general(a, b, (((1,), (1,)), ((), ())), preferred_element_type=F32)


def iota(shape, dim):
    return lax.broadcasted_iota(jnp.int32, shape, dim)


def even_lanes(shape):
    return (iota(shape, 1) & 1) == 0


def split(x):
    high = x.astype(BF16)
    return high, (x - high.astype(F32)).astype(BF16)


def strided(ref, rows):
    return jnp.concatenate([ref[k, rows, :] for k in range(TILES)], axis=1)


def lane_up(x):
    return pltpu.roll(x, 1, 1)


def lane_down(x):
    return pltpu.roll(x, LANES - 1, 1)


def kernel(
    chans,
    volt, w_hbm, sat_hbm, offs_hbm, ang_hbm,
    wide, w_out,
    x, w_in, sat_in, offs, ang, we, sat_l, sat_r, steer, vv, pack, packed, halo_l, halo_r, ana, syn, nul, stage, sbuf, recv,
    in_sem, x_sem, sat_ssem, sat_rsem, halo_ssem, halo_rsem, beam_ssem, beam_rsem,
):
    me = lax.axis_index("chan")
    sec = lax.axis_index("section")
    left = lax.rem(me + chans - 1, chans)
    right = lax.rem(me + 1, chans)

    def load(c, d, z):
        return pltpu.make_async_copy(
            volt.at[c, z, d],
            x.at[c, d, pl.ds(0, ROWS), pl.ds(z * TIME, TIME)],
            x_sem.at[c, d, z],
        )

    sat_l[...] = jnp.zeros_like(sat_l)
    sat_r[...] = jnp.zeros_like(sat_r)
    halo_l[...] = jnp.zeros_like(halo_l)
    halo_r[...] = jnp.zeros_like(halo_r)

    barrier = pltpu.get_barrier_semaphore()
    for j in range(1, SEC):
        pl.semaphore_signal(
            barrier, inc=1, device_id={"section": lax.rem(sec + j, SEC)}, device_id_type=MESH
        )
    sides = ((me > 0, left), (me < chans - 1, right))
    for exists, peer in sides:

        @pl.when(exists)
        def _():
            pl.semaphore_signal(barrier, inc=1, device_id={"chan": peer}, device_id_type=MESH)

    small = [
        pltpu.make_async_copy(source, target, in_sem.at[i])
        for i, (source, target) in enumerate(
            ((ang_hbm, ang), (w_hbm, w_in), (sat_hbm, sat_in), (offs_hbm, offs))
        )
    ]
    for copy in small:
        copy.start()
    for c in range(CYC):
        for d in range(DISH):
            for z in range(2):
                load(c, d, z).start()

    def sat_copy(side):
        return pltpu.make_async_remote_copy(
            src_ref=sat_in,
            dst_ref=sat_r if side == 0 else sat_l,
            send_sem=sat_ssem.at[side],
            recv_sem=sat_rsem.at[side],
            device_id={"chan": left if side == 0 else right},
            device_id_type=MESH,
        )

    pl.semaphore_wait(barrier, SEC - 1 + sum(e.astype(jnp.int32) for e, _peer in sides))
    small[2].wait()
    for side in range(2):

        @pl.when(sides[side][0])
        def _():
            sat_copy(side).start()

    spread = (lax.shift_right_logical(iota((PORT, LANES), 1), 1) == iota((PORT, LANES), 0)).astype(
        F32
    ).astype(BF16)
    own = (iota((WR, LANES), 0) & 1) == (iota((WR, LANES), 1) & 1)
    for c in range(CYC):
        for d in range(DISH):
            x[c, d, pl.ds(ROWS, LANES - ROWS), :] = jnp.zeros((LANES - ROWS, 2 * TIME), BF16)
    wide[:, pl.ds(ALL * PER, (ALLP - ALL) * PER), :] = jnp.zeros(
        (2 * CYC, (ALLP - ALL) * PER, TIME), F32
    )
    small[0].wait()
    grown_table = []
    for values in (jnp.cos(ang[...]), jnp.sin(ang[...])):
        for part in split(values):
            grown_table.append(dot(part, spread).astype(BF16))
    small[1].wait()
    for d in range(DISH):
        for z in range(2):
            grown = dot(w_in[z, d].reshape(WR, PORT), spread)
            we[d, pl.ds(z * WR, WR), :] = jnp.where(own, grown, 0.0).astype(BF16)

    def beams(c, k):
        dishes = range(PART * k, PART * (k + 1))
        if c == 1:
            project(dishes)
        for j, d in enumerate(dishes):
            if c == 0:
                load(c, d, 0).wait()
                load(c, d, 1).wait()
            both = dot(we[d], x[c, d])
            real = both[:WR, :TIME] + both[WR:, TIME:]
            imag = both[:WR, TIME:] - both[WR:, :TIME]
            for s in range(SEC):
                rows = pl.ds(j * PER, PER)
                stage[s, k, rows, pl.ds(0, TIME)] = real[s * PER : (s + 1) * PER]
                stage[s, k, rows, pl.ds(TIME, TIME)] = imag[s * PER : (s + 1) * PER]
        for s in range(SEC):
            sbuf[c, s, k] = stage[s, k].astype(BF16)

    def beam_copy(c, k, j):
        peer = lax.rem(sec + j, SEC)
        return pltpu.make_async_remote_copy(
            src_ref=sbuf.at[c, peer, k],
            dst_ref=recv.at[c, sec, k],
            send_sem=beam_ssem.at[c, k, j - 1],
            recv_sem=beam_rsem.at[c, k, j - 1],
            device_id={"section": peer},
            device_id_type=MESH,
        )

    def send_beams(c, k):
        for j in (2, 3, 1):
            beam_copy(c, k, j).start()
        recv[c, sec, k] = sbuf[c, sec, k]

    for k in range(PARTS):
        beams(0, k)
        send_beams(0, k)

    for side in range(2):

        @pl.when(sides[1 - side][0])
        def _():
            sat_copy(side).wait_recv()

    row = iota((8, TIME), 0)
    keep = (iota((8, LANES), 0) >= 4) == ((iota((8, LANES), 1) & 1) == 1)
    for c in range(CYC):
        own_s, left_s, right_s = (
            jnp.where((row & 1) == 0, ref[pl.ds(c, 1), pl.ds(0, 1)], ref[pl.ds(c, 1), pl.ds(1, 1)])
            for ref in (sat_in, sat_l, sat_r)
        )
        index = jnp.where((row & 3) < 2, own_s, jnp.where(row < 4, left_s, right_s))
        hot = (index == iota((8, TIME), 1)).astype(F32).astype(BF16)[:, :64]
        parts = [dot(hot, part) for part in grown_table]
        for i, (h, l) in enumerate(((0, 1), (2, 3))):
            steer[c, i] = parts[h] + parts[l]
        stacked = [jnp.where(keep, parts[i], 0.0) for i in (0, 2, 1, 3)]
        for i in range(4):
            ana[c, pl.ds(8 * i, 8), :] = stacked[i]

    even4 = even_lanes((4, LANES))

    def null_vectors(c):
        if c == 0:
            small[3].wait()
        times = (offs[pl.ds(c, 1), :] == iota((TIME, TIME), 0)).astype(F32).astype(BF16)
        count = dot_t(jnp.ones((8, TIME), BF16), times)
        probe = ana[c].astype(BF16)
        for d in range(DISH):
            if c == 1:
                load(c, d, 0).wait()
                load(c, d, 1).wait()
            block = x[c, d]
            out = dot(probe, block)
            out = out[:16] + out[16:]
            y_real = (out[:8, :TIME] + out[8:, TIME:]) * count
            y_imag = (out[8:, :TIME] - out[:8, TIME:]) * count
            lines = jnp.concatenate(
                [
                    jnp.concatenate([y_real, -y_imag], axis=1),
                    jnp.concatenate([y_imag, y_real], axis=1),
                ],
                axis=0,
            )
            high, low = split(lines)
            back = dot_t(jnp.concatenate([high, low], axis=0), block)
            back = back[:16] + back[16:]
            for i in range(2):
                kept = jnp.where(even4, back[8 * i : 8 * i + 4], back[8 * i + 4 : 8 * i + 8])
                for k in range(TILES):
                    vv[c, k, pl.ds(8 * d + 4 * i, 4), :] = kept[:, k * TIME : (k + 1) * TIME]

    even = even_lanes((DISH, LANES))

    def halo_copy(c, side):
        return pltpu.make_async_remote_copy(
            src_ref=packed.at[c, side],
            dst_ref=(halo_r if side == 0 else halo_l).at[c],
            send_sem=halo_ssem.at[c, side],
            recv_sem=halo_rsem.at[c, side],
            device_id={"chan": left if side == 0 else right},
            device_id_type=MESH,
        )

    def take(c, q):
        return strided(vv.at[c], pl.ds(q, DISH, stride=8))

    def send_halo(c):
        for i in range(2):
            first, second = take(c, 4 * i + 2), take(c, 4 * i + 3)
            rows = pl.ds(i * DISH, DISH)
            pack[0, rows, :] = jnp.where(even, first, lane_up(second))
            pack[1, rows, :] = jnp.where(even, lane_down(first), second)
        packed[c] = pack[...]
        for side in range(2):

            @pl.when(sides[side][0])
            def _():
                halo_copy(c, side).start()

    pack[...] = jnp.zeros_like(pack)
    null_vectors(0)
    send_halo(0)
    null_vectors(1)
    send_halo(1)

    def lane_sum(v):
        e = jnp.sum(jnp.where(even, v, 0.0), axis=1, keepdims=True)
        o = jnp.sum(jnp.where(even, 0.0, v), axis=1, keepdims=True)
        return jnp.where(even, e, o)

    def project_vectors(c):
        for side in range(2):

            @pl.when(sides[1 - side][0])
            def _():
                halo_copy(c, side).wait_recv()

        u = []
        halos = [ref[c] for ref in (halo_l, halo_r)]
        for i in range(2):
            from_l, from_r = (h[i * DISH : (i + 1) * DISH] for h in halos)
            halo = (
                jnp.where(even, from_l, lane_up(from_r)),
                jnp.where(even, lane_down(from_l), from_r),
            )
            for s in range(2):
                v = take(c, 4 * i + s)
                v = v + jnp.where(even, lane_down(v), lane_up(v))
                u.append(v + halo[s] + LOADING * steer[c, i, pl.ds(s, 1), :])
        u0r, u1r, u0i, u1i = u
        inv0 = 1.0 / lane_sum(u0r * u0r + u0i * u0i)
        inv1 = 1.0 / lane_sum(u1r * u1r + u1i * u1i)
        t0r, t0i = u0r * inv0, u0i * inv0
        kr = lane_sum(t0r * u1r + t0i * u1i)
        ki = lane_sum(t0r * u1i - t0i * u1r)
        t1r = (u1r - (u0r * kr - u0i * ki)) * inv1
        t1i = (u1i - (u0r * ki + u0i * kr)) * inv1
        for q, (t, v) in enumerate(((t0r, u0r), (t0i, u0i), (t1r, u1r), (t1i, u1i))):
            for k in range(TILES):
                syn[k, pl.ds(16 * q, DISH), :] = t[:, k * TIME : (k + 1) * TIME]
            nul[pl.ds(16 * q, DISH), :] = v

    def project(dishes):
        inner = []
        for d in dishes:
            high, low = split(strided(syn, pl.ds(d, 4, stride=16)))
            old = we[d]
            inner.append(dot_t(old, high) + dot_t(old, low))
        for d, g in zip(dishes, inner):
            gr, gi = g[:WR], g[WR:]
            v = [nul[pl.ds(16 * q + d, 1), :] for q in range(4)]
            new_r = we[d, pl.ds(0, WR), :].astype(F32)
            new_i = we[d, pl.ds(WR, WR), :].astype(F32)
            for s in range(2):
                cr = gr[:, 2 * s : 2 * s + 1] + gi[:, 2 * s + 1 : 2 * s + 2]
                ci = gi[:, 2 * s : 2 * s + 1] - gr[:, 2 * s + 1 : 2 * s + 2]
                vr, vi = v[2 * s], v[2 * s + 1]
                new_r = new_r - (vr * cr - vi * ci)
                new_i = new_i - (vr * ci + vi * cr)
            we[d, pl.ds(0, WR), :] = jnp.where(own, new_r, 0.0).astype(BF16)
            we[d, pl.ds(WR, WR), :] = jnp.where(own, new_i, 0.0).astype(BF16)

    project_vectors(0)
    for k in range(PARTS):
        beams(1, k)
        send_beams(1, k)

    project_vectors(1)
    gather = (lax.shift_right_logical(iota((LANES, PORT), 0), 1) == iota((LANES, PORT), 1)).astype(
        F32
    ).astype(BF16)
    for k in range(PARTS):
        project(range(PART * k, PART * (k + 1)))
    for d in range(DISH):
        for z in range(2):
            dense = dot(we[d, pl.ds(z * WR, WR), :], gather).astype(BF16)
            w_out[z, d] = dense.reshape(BEAM, CH, PORT)

    for c in range(CYC):
        for k in range(PARTS):
            for j in range(1, SEC):
                beam_copy(c, k, j).wait_recv()
            for s in range(SEC):
                block = recv[c, s, k].astype(F32)[:BLK]
                rows = pl.ds((s * PARTS + k) * BLK, BLK)
                for z in range(2):
                    wide[2 * c + z, rows, :] = block[:, z * TIME : (z + 1) * TIME]

    for c in range(CYC):
        for k in range(PARTS):
            for j in range(1, SEC):
                beam_copy(c, k, j).wait_send()
    for side in range(2):

        @pl.when(sides[side][0])
        def _():
            sat_copy(side).wait_send()
            for c in range(CYC):
                halo_copy(c, side).wait_send()


def correlate(wide, w_new, vis_hbm, w_hbm, vis, flat, corr, sems):
    weights = pltpu.make_async_copy(w_new, w_hbm, sems.at[0])
    weights.start()
    for r in range(PER):
        lanes = [wide[k, pl.ds(r, ALLP, stride=PER), :] for k in range(2 * CYC)]
        straight = jnp.concatenate(lanes, axis=1)
        turned = jnp.concatenate([lanes[1], -lanes[0], lanes[3], -lanes[2]], axis=1)
        right_side = straight.astype(BF16)
        result = dot_t(jnp.concatenate([straight, turned], axis=0).astype(BF16), right_side)
        result = result * (1.0 / (CYC * TIME))
        for z in range(2):
            corr[z, pl.ds(r * ALLP, ALLP), pl.ds(0, ALLP)] = result[z * ALLP : (z + 1) * ALLP]
    for z in range(2):
        for d in range(ALL):
            flat[z, :, pl.ds(d * ALL, ALL)] = corr[z, pl.ds(d, PER, stride=ALLP), :][:, :ALL]
        vis[z] = flat[z].reshape(DISH, CH, ALL * ALL)
        pltpu.make_async_copy(vis.at[z], vis_hbm.at[z], sems.at[1 + z]).start()
    weights.wait()
    for z in range(2):
        pltpu.make_async_copy(vis.at[z], vis_hbm.at[z], sems.at[1 + z]).wait()


def per_device(chans, voltages, weights, sat_index, offsets, angles):
    volt = voltages.transpose(0, 1, 2, 4, 3, 5).reshape(CYC, 2, DISH, ROWS, TIME)
    w_in = weights.transpose(0, 1, 3, 2, 4)
    sat = sat_index.reshape(CYC, 2)
    vmem = pl.BlockSpec(memory_space=pltpu.VMEM)
    hbm = pl.BlockSpec(memory_space=pltpu.HBM)
    dma = pltpu.SemaphoreType.DMA
    wide, new = pl.pallas_call(
        functools.partial(kernel, chans),
        out_shape=(
            jax.ShapeDtypeStruct((2 * CYC, ALLP * PER, TIME), F32),
            jax.ShapeDtypeStruct((2, DISH, BEAM, CH, PORT), BF16),
        ),
        in_specs=[hbm] * 5,
        out_specs=(vmem, vmem),
        scratch_shapes=[
            pltpu.VMEM((CYC, DISH, LANES, 2 * TIME), BF16),
            pltpu.VMEM((2, DISH, BEAM, CH, PORT), BF16),
            pltpu.VMEM((CYC, 2), jnp.int32),
            pltpu.VMEM((CYC, TIME), jnp.int32),
            pltpu.VMEM((64, PORT), F32),
            pltpu.VMEM((DISH, 2 * WR, LANES), BF16),
            pltpu.VMEM((CYC, 2), jnp.int32),
            pltpu.VMEM((CYC, 2), jnp.int32),
            pltpu.VMEM((CYC, 2, 8, LANES), F32),
            pltpu.VMEM((CYC, TILES, DISH * 8, TIME), F32),
            pltpu.VMEM((2, 24, LANES), F32),
            pltpu.VMEM((CYC, 2, 24, LANES), F32),
            pltpu.VMEM((CYC, 24, LANES), F32),
            pltpu.VMEM((CYC, 24, LANES), F32),
            pltpu.VMEM((CYC, 32, LANES), F32),
            pltpu.VMEM((TILES, 64, TIME), F32),
            pltpu.VMEM((64, LANES), F32),
            pltpu.VMEM((SEC, PARTS, BLKP, 2 * TIME), F32),
            pltpu.VMEM((CYC, SEC, PARTS, BLKP, 2 * TIME), BF16),
            pltpu.VMEM((CYC, SEC, PARTS, BLKP, 2 * TIME), BF16),
            dma((4,)),
            dma((CYC, DISH, 2)),
            dma((2,)),
            dma((2,)),
            dma((CYC, 2)),
            dma((CYC, 2)),
            dma((CYC, PARTS, SEC - 1)),
            dma((CYC, PARTS, SEC - 1)),
        ],
        compiler_params=pltpu.CompilerParams(
            collective_id=0, has_side_effects=True, vmem_limit_bytes=24 << 20
        ),
    )(*(pltpu.with_memory_space_constraint(a, pltpu.HBM) for a in (volt, w_in, sat, offsets, angles)))
    vis, new = pl.pallas_call(
        correlate,
        out_shape=(
            jax.ShapeDtypeStruct((2, DISH, CH, ALL * ALL), F32),
            jax.ShapeDtypeStruct((2, DISH, BEAM, CH, PORT), BF16),
        ),
        in_specs=[vmem, vmem],
        out_specs=(hbm, hbm),
        scratch_shapes=[
            pltpu.VMEM((2, DISH, CH, ALL * ALL), F32),
            pltpu.VMEM((2, PER, ALL * ALL), F32),
            pltpu.VMEM((2, PER * ALLP, TIME), F32),
            dma((3,)),
        ],
        compiler_params=pltpu.CompilerParams(vmem_limit_bytes=24 << 20),
    )(wide, new)
    return vis, new.transpose(0, 1, 3, 2, 4)


def solution(mesh):
    placed = (
        P(None, None, "section", "chan", None, None),
        P(None, "section", "chan", None, None),
        P(None, "chan", None),
        P(),
        P(),
    )
    return jax.shard_map(
        functools.partial(per_device, mesh.shape["chan"]),
        mesh=mesh,
        in_specs=placed,
        out_specs=(P(None, "section", "chan", None), P(None, "section", "chan", None, None)),
        check_vma=False,
    )
```

```python
import functools

import jax
import jax.numpy as jnp
from jax import lax
from jax.experimental import pallas as pl
from jax.experimental.pallas import tpu as pltpu
from jax.sharding import PartitionSpec as P

LOADING = 100.0
MESH = pl.DeviceIdType.MESH
F32 = jnp.float32
BF16 = jnp.bfloat16
CYC, DISH, CH, BEAM, PORT, TIME = 2, 9, 2, 36, 188, 128
SEC = 4
ROWS = CH * PORT
LANES = 384
TILES = LANES // TIME
WR = BEAM * CH
PER = WR // SEC
PARTS = 3
PART = DISH // PARTS
BLK = PART * PER
BLKP = 56
ALL = SEC * DISH
ALLP = 40


def dot(a, b):
    return lax.dot_general(a, b, (((1,), (0,)), ((), ())), preferred_element_type=F32)


def dot_t(a, b):
    return lax.dot_general(a, b, (((1,), (1,)), ((), ())), preferred_element_type=F32)


def iota(shape, dim):
    return lax.broadcasted_iota(jnp.int32, shape, dim)


def even_lanes(shape):
    return (iota(shape, 1) & 1) == 0


def split(x):
    high = x.astype(BF16)
    return high, (x - high.astype(F32)).astype(BF16)


def strided(ref, rows):
    return jnp.concatenate([ref[k, rows, :] for k in range(TILES)], axis=1)


def lane_up(x):
    return pltpu.roll(x, 1, 1)


def lane_down(x):
    return pltpu.roll(x, LANES - 1, 1)


def kernel(
    chans,
    volt, w_hbm, sat_hbm, offs_hbm, ang_hbm,
    wide, w_out,
    x, w_in, sat_in, offs, ang, we, sat_l, sat_r, steer, vv, pack, packed, halo_l, halo_r, ana, syn, nul, stage, sbuf, recv,
    in_sem, x_sem, sat_ssem, sat_rsem, halo_ssem, halo_rsem, beam_ssem, beam_rsem,
):
    me = lax.axis_index("chan")
    sec = lax.axis_index("section")
    left = lax.rem(me + chans - 1, chans)
    right = lax.rem(me + 1, chans)

    def load(c, d, z):
        return pltpu.make_async_copy(
            volt.at[c, z, d],
            x.at[c, z, d, pl.ds(0, ROWS)],
            x_sem.at[c, d, z],
        )

    def wait_voltages(c):
        for d in range(DISH):
            for z in range(2):
                load(c, d, z).wait()

    def voltage(c, d):
        return jnp.concatenate([x[c, 0, d], x[c, 1, d]], axis=1)

    sat_l[...] = jnp.zeros_like(sat_l)
    sat_r[...] = jnp.zeros_like(sat_r)
    halo_l[...] = jnp.zeros_like(halo_l)
    halo_r[...] = jnp.zeros_like(halo_r)

    barrier = pltpu.get_barrier_semaphore()
    for j in range(1, SEC):
        pl.semaphore_signal(
            barrier, inc=1, device_id={"section": lax.rem(sec + j, SEC)}, device_id_type=MESH
        )
    sides = ((me > 0, left), (me < chans - 1, right))
    for exists, peer in sides:

        @pl.when(exists)
        def _():
            pl.semaphore_signal(barrier, inc=1, device_id={"chan": peer}, device_id_type=MESH)

    small = [
        pltpu.make_async_copy(source, target, in_sem.at[i])
        for i, (source, target) in enumerate(
            ((ang_hbm, ang), (w_hbm, w_in), (sat_hbm, sat_in), (offs_hbm, offs))
        )
    ]
    for copy in small:
        copy.start()
    for c in range(CYC):
        for d in range(DISH):
            for z in range(2):
                load(c, d, z).start()

    def sat_copy(side):
        return pltpu.make_async_remote_copy(
            src_ref=sat_in,
            dst_ref=sat_r if side == 0 else sat_l,
            send_sem=sat_ssem.at[side],
            recv_sem=sat_rsem.at[side],
            device_id={"chan": left if side == 0 else right},
            device_id_type=MESH,
        )

    pl.semaphore_wait(barrier, SEC - 1 + sum(e.astype(jnp.int32) for e, _peer in sides))
    small[2].wait()
    for side in range(2):

        @pl.when(sides[side][0])
        def _():
            sat_copy(side).start()

    spread = (lax.shift_right_logical(iota((PORT, LANES), 1), 1) == iota((PORT, LANES), 0)).astype(
        F32
    ).astype(BF16)
    own = (iota((WR, LANES), 0) & 1) == (iota((WR, LANES), 1) & 1)
    for c in range(CYC):
        for d in range(DISH):
            for z in range(2):
                x[c, z, d, pl.ds(ROWS, LANES - ROWS), :] = jnp.zeros((LANES - ROWS, TIME), BF16)
    wide[:, pl.ds(ALL * PER, (ALLP - ALL) * PER), :] = jnp.zeros(
        (2 * CYC, (ALLP - ALL) * PER, TIME), F32
    )
    small[0].wait()
    grown_table = []
    for values in (jnp.cos(ang[...]), jnp.sin(ang[...])):
        for part in split(values):
            grown_table.append(dot(part, spread).astype(BF16))
    small[1].wait()
    for d in range(DISH):
        for z in range(2):
            grown = dot(w_in[z, d].reshape(WR, PORT), spread)
            we[d, pl.ds(z * WR, WR), :] = jnp.where(own, grown, 0.0).astype(BF16)

    def beams(c, k):
        dishes = range(PART * k, PART * (k + 1))
        if c == 1:
            project(dishes)
        for j, d in enumerate(dishes):
            both = dot(we[d], voltage(c, d))
            real = both[:WR, :TIME] + both[WR:, TIME:]
            imag = both[:WR, TIME:] - both[WR:, :TIME]
            for s in range(SEC):
                rows = pl.ds(j * PER, PER)
                stage[s, k, rows, pl.ds(0, TIME)] = real[s * PER : (s + 1) * PER]
                stage[s, k, rows, pl.ds(TIME, TIME)] = imag[s * PER : (s + 1) * PER]
        for s in range(SEC):
            sbuf[c, s, k] = stage[s, k].astype(BF16)

    def beam_copy(c, k, j):
        peer = lax.rem(sec + j, SEC)
        return pltpu.make_async_remote_copy(
            src_ref=sbuf.at[c, peer, k],
            dst_ref=recv.at[c, sec, k],
            send_sem=beam_ssem.at[c, k, j - 1],
            recv_sem=beam_rsem.at[c, k, j - 1],
            device_id={"section": peer},
            device_id_type=MESH,
        )

    def send_beams(c, k):
        for j in (2, 3, 1):
            beam_copy(c, k, j).start()
        recv[c, sec, k] = sbuf[c, sec, k]

    wait_voltages(0)
    for k in range(PARTS):
        beams(0, k)
        send_beams(0, k)

    for side in range(2):

        @pl.when(sides[1 - side][0])
        def _():
            sat_copy(side).wait_recv()

    row = iota((8, TIME), 0)
    keep = (iota((8, LANES), 0) >= 4) == ((iota((8, LANES), 1) & 1) == 1)
    for c in range(CYC):
        own_s, left_s, right_s = (
            jnp.where((row & 1) == 0, ref[pl.ds(c, 1), pl.ds(0, 1)], ref[pl.ds(c, 1), pl.ds(1, 1)])
            for ref in (sat_in, sat_l, sat_r)
        )
        index = jnp.where((row & 3) < 2, own_s, jnp.where(row < 4, left_s, right_s))
        hot = (index == iota((8, TIME), 1)).astype(F32).astype(BF16)[:, :64]
        parts = [dot(hot, part) for part in grown_table]
        for i, (h, l) in enumerate(((0, 1), (2, 3))):
            steer[c, i] = parts[h] + parts[l]
        stacked = [jnp.where(keep, parts[i], 0.0) for i in (0, 2, 1, 3)]
        for i in range(4):
            ana[c, pl.ds(8 * i, 8), :] = stacked[i]

    even4 = even_lanes((4, LANES))

    def null_vectors(c):
        if c == 0:
            small[3].wait()
        times = (offs[pl.ds(c, 1), :] == iota((TIME, TIME), 0)).astype(F32).astype(BF16)
        count = dot_t(jnp.ones((8, TIME), BF16), times)
        probe = ana[c].astype(BF16)
        for first in range(0, DISH, 9):
            dishes = range(first, first + 9)
            outs = [dot(probe, voltage(c, d)) for d in dishes]
            lines = []
            for out in outs:
                out = out[:16] + out[16:]
                y_real = (out[:8, :TIME] + out[8:, TIME:]) * count
                y_imag = (out[8:, :TIME] - out[:8, TIME:]) * count
                pair = jnp.concatenate(
                    [
                        jnp.concatenate([y_real, -y_imag], axis=1),
                        jnp.concatenate([y_imag, y_real], axis=1),
                    ],
                    axis=0,
                )
                lines.append(jnp.concatenate(split(pair), axis=0))
            backs = []
            for j, d in enumerate(dishes):
                block = voltage(c, d)
                backs.append(dot_t(lines[j], block))
            for d, back in zip(dishes, backs):
                back = back[:16] + back[16:]
                for i in range(2):
                    kept = jnp.where(even4, back[8 * i : 8 * i + 4], back[8 * i + 4 : 8 * i + 8])
                    for k in range(TILES):
                        vv[c, k, pl.ds(8 * d + 4 * i, 4), :] = kept[:, k * TIME : (k + 1) * TIME]

    even = even_lanes((DISH, LANES))

    def halo_copy(c, side):
        return pltpu.make_async_remote_copy(
            src_ref=packed.at[c, side],
            dst_ref=(halo_r if side == 0 else halo_l).at[c],
            send_sem=halo_ssem.at[c, side],
            recv_sem=halo_rsem.at[c, side],
            device_id={"chan": left if side == 0 else right},
            device_id_type=MESH,
        )

    def take(c, q):
        return strided(vv.at[c], pl.ds(q, DISH, stride=8))

    def send_halo(c):
        for i in range(2):
            first, second = take(c, 4 * i + 2), take(c, 4 * i + 3)
            rows = pl.ds(i * DISH, DISH)
            pack[0, rows, :] = jnp.where(even, first, lane_up(second))
            pack[1, rows, :] = jnp.where(even, lane_down(first), second)
        packed[c] = pack[...]
        for side in range(2):

            @pl.when(sides[side][0])
            def _():
                halo_copy(c, side).start()

    pack[...] = jnp.zeros_like(pack)
    null_vectors(0)
    send_halo(0)
    wait_voltages(1)
    null_vectors(1)
    send_halo(1)

    def lane_sum(v):
        e = jnp.sum(jnp.where(even, v, 0.0), axis=1, keepdims=True)
        o = jnp.sum(jnp.where(even, 0.0, v), axis=1, keepdims=True)
        return jnp.where(even, e, o)

    def project_vectors(c):
        for side in range(2):

            @pl.when(sides[1 - side][0])
            def _():
                halo_copy(c, side).wait_recv()

        u = []
        halos = [ref[c] for ref in (halo_l, halo_r)]
        for i in range(2):
            from_l, from_r = (h[i * DISH : (i + 1) * DISH] for h in halos)
            halo = (
                jnp.where(even, from_l, lane_up(from_r)),
                jnp.where(even, lane_down(from_l), from_r),
            )
            for s in range(2):
                v = take(c, 4 * i + s)
                v = v + jnp.where(even, lane_down(v), lane_up(v))
                u.append(v + halo[s] + LOADING * steer[c, i, pl.ds(s, 1), :])
        u0r, u1r, u0i, u1i = u
        inv0 = 1.0 / lane_sum(u0r * u0r + u0i * u0i)
        inv1 = 1.0 / lane_sum(u1r * u1r + u1i * u1i)
        t0r, t0i = u0r * inv0, u0i * inv0
        kr = lane_sum(t0r * u1r + t0i * u1i)
        ki = lane_sum(t0r * u1i - t0i * u1r)
        t1r = (u1r - (u0r * kr - u0i * ki)) * inv1
        t1i = (u1i - (u0r * ki + u0i * kr)) * inv1
        for q, (t, v) in enumerate(((t0r, u0r), (t0i, u0i), (t1r, u1r), (t1i, u1i))):
            for k in range(TILES):
                syn[k, pl.ds(16 * q, DISH), :] = t[:, k * TIME : (k + 1) * TIME]
                nul[k, pl.ds(16 * q, DISH), :] = v[:, k * TIME : (k + 1) * TIME]

    def project(dishes):
        inner, bases, changes = [], [], []
        for d in dishes:
            probe = jnp.concatenate(split(strided(syn, pl.ds(d, 4, stride=16))), axis=0)
            inner.append([dot_t(probe, we[d, pl.ds(z * WR, WR), :]) for z in range(2)])
        for d in dishes:
            high, low = split(strided(nul, pl.ds(d, 4, stride=16)))
            bases.append(jnp.concatenate([high, low, high], axis=0))
        for outs, basis in zip(inner, bases):
            gr, gi = (out[:4] + out[4:] for out in outs)
            first, second = [], []
            for s in range(2):
                cr = gr[2 * s : 2 * s + 1] + gi[2 * s + 1 : 2 * s + 2]
                ci = gi[2 * s : 2 * s + 1] - gr[2 * s + 1 : 2 * s + 2]
                first += [cr, -ci]
                second += [ci, cr]
            for rows in (first, second):
                c_high, c_low = split(jnp.concatenate(rows, axis=0))
                amount = jnp.concatenate([c_high, c_high, c_low], axis=0)
                changes.append(
                    lax.dot_general(
                        amount, basis, (((0,), (0,)), ((), ())), preferred_element_type=F32
                    )
                )
        for d in dishes:
            for z in range(2):
                new = we[d, pl.ds(z * WR, WR), :].astype(F32) - changes.pop(0)
                we[d, pl.ds(z * WR, WR), :] = jnp.where(own, new, 0.0).astype(BF16)

    project_vectors(0)
    for k in range(PARTS):
        beams(1, k)
        send_beams(1, k)

    project_vectors(1)
    gather = (lax.shift_right_logical(iota((LANES, PORT), 0), 1) == iota((LANES, PORT), 1)).astype(
        F32
    ).astype(BF16)
    for k in range(PARTS):
        project(range(PART * k, PART * (k + 1)))
    for d in range(DISH):
        for z in range(2):
            dense = dot(we[d, pl.ds(z * WR, WR), :], gather).astype(BF16)
            w_out[z, d] = dense.reshape(BEAM, CH, PORT)

    for c in range(CYC):
        for k in range(PARTS):
            for j in range(1, SEC):
                beam_copy(c, k, j).wait_recv()
            for s in range(SEC):
                block = recv[c, s, k].astype(F32)[:BLK]
                rows = pl.ds((s * PARTS + k) * BLK, BLK)
                for z in range(2):
                    wide[2 * c + z, rows, :] = block[:, z * TIME : (z + 1) * TIME]

    for c in range(CYC):
        for k in range(PARTS):
            for j in range(1, SEC):
                beam_copy(c, k, j).wait_send()
    for side in range(2):

        @pl.when(sides[side][0])
        def _():
            sat_copy(side).wait_send()
            for c in range(CYC):
                halo_copy(c, side).wait_send()


def correlate(wide, w_new, vis_hbm, w_hbm, vis, flat, corr, sems):
    weights = pltpu.make_async_copy(w_new, w_hbm, sems.at[0])
    weights.start()
    for r in range(PER):
        lanes = [wide[k, pl.ds(r, ALLP, stride=PER), :] for k in range(2 * CYC)]
        straight = jnp.concatenate(lanes, axis=1)
        turned = jnp.concatenate([lanes[1], -lanes[0], lanes[3], -lanes[2]], axis=1)
        right_side = straight.astype(BF16)
        result = dot_t(jnp.concatenate([straight, turned], axis=0).astype(BF16), right_side)
        result = result * (1.0 / (CYC * TIME))
        for z in range(2):
            corr[z, pl.ds(r * ALLP, ALLP), pl.ds(0, ALLP)] = result[z * ALLP : (z + 1) * ALLP]
    for z in range(2):
        for d in range(ALL):
            flat[z, :, pl.ds(d * ALL, ALL)] = corr[z, pl.ds(d, PER, stride=ALLP), :][:, :ALL]
        vis[z] = flat[z].reshape(DISH, CH, ALL * ALL)
        pltpu.make_async_copy(vis.at[z], vis_hbm.at[z], sems.at[1 + z]).start()
    weights.wait()
    for z in range(2):
        pltpu.make_async_copy(vis.at[z], vis_hbm.at[z], sems.at[1 + z]).wait()


def per_device(chans, voltages, weights, sat_index, offsets, angles):
    volt = voltages.transpose(0, 1, 2, 4, 3, 5).reshape(CYC, 2, DISH, ROWS, TIME)
    w_in = weights.transpose(0, 1, 3, 2, 4)
    sat = sat_index.reshape(CYC, 2)
    vmem = pl.BlockSpec(memory_space=pltpu.VMEM)
    hbm = pl.BlockSpec(memory_space=pltpu.HBM)
    dma = pltpu.SemaphoreType.DMA
    wide, new = pl.pallas_call(
        functools.partial(kernel, chans),
        out_shape=(
            jax.ShapeDtypeStruct((2 * CYC, ALLP * PER, TIME), F32),
            jax.ShapeDtypeStruct((2, DISH, BEAM, CH, PORT), BF16),
        ),
        in_specs=[hbm] * 5,
        out_specs=(vmem, vmem),
        scratch_shapes=[
            pltpu.VMEM((CYC, 2, DISH, LANES, TIME), BF16),
            pltpu.VMEM((2, DISH, BEAM, CH, PORT), BF16),
            pltpu.VMEM((CYC, 2), jnp.int32),
            pltpu.VMEM((CYC, TIME), jnp.int32),
            pltpu.VMEM((64, PORT), F32),
            pltpu.VMEM((DISH, 2 * WR, LANES), BF16),
            pltpu.VMEM((CYC, 2), jnp.int32),
            pltpu.VMEM((CYC, 2), jnp.int32),
            pltpu.VMEM((CYC, 2, 8, LANES), F32),
            pltpu.VMEM((CYC, TILES, DISH * 8, TIME), F32),
            pltpu.VMEM((2, 24, LANES), F32),
            pltpu.VMEM((CYC, 2, 24, LANES), F32),
            pltpu.VMEM((CYC, 24, LANES), F32),
            pltpu.VMEM((CYC, 24, LANES), F32),
            pltpu.VMEM((CYC, 32, LANES), F32),
            pltpu.VMEM((TILES, 64, TIME), F32),
            pltpu.VMEM((TILES, 64, TIME), F32),
            pltpu.VMEM((SEC, PARTS, BLKP, 2 * TIME), F32),
            pltpu.VMEM((CYC, SEC, PARTS, BLKP, 2 * TIME), BF16),
            pltpu.VMEM((CYC, SEC, PARTS, BLKP, 2 * TIME), BF16),
            dma((4,)),
            dma((CYC, DISH, 2)),
            dma((2,)),
            dma((2,)),
            dma((CYC, 2)),
            dma((CYC, 2)),
            dma((CYC, PARTS, SEC - 1)),
            dma((CYC, PARTS, SEC - 1)),
        ],
        compiler_params=pltpu.CompilerParams(
            collective_id=0, has_side_effects=True, vmem_limit_bytes=24 << 20
        ),
    )(*(pltpu.with_memory_space_constraint(a, pltpu.HBM) for a in (volt, w_in, sat, offsets, angles)))
    vis, new = pl.pallas_call(
        correlate,
        out_shape=(
            jax.ShapeDtypeStruct((2, DISH, CH, ALL * ALL), F32),
            jax.ShapeDtypeStruct((2, DISH, BEAM, CH, PORT), BF16),
        ),
        in_specs=[vmem, vmem],
        out_specs=(hbm, hbm),
        scratch_shapes=[
            pltpu.VMEM((2, DISH, CH, ALL * ALL), F32),
            pltpu.VMEM((2, PER, ALL * ALL), F32),
            pltpu.VMEM((2, PER * ALLP, TIME), F32),
            dma((3,)),
        ],
        compiler_params=pltpu.CompilerParams(vmem_limit_bytes=24 << 20),
    )(wide, new)
    return vis, new.transpose(0, 1, 3, 2, 4)


def solution(mesh):
    placed = (
        P(None, None, "section", "chan", None, None),
        P(None, "section", "chan", None, None),
        P(None, "chan", None),
        P(),
        P(),
    )
    return jax.shard_map(
        functools.partial(per_device, mesh.shape["chan"]),
        mesh=mesh,
        in_specs=placed,
        out_specs=(P(None, "section", "chan", None), P(None, "section", "chan", None, None)),
        check_vma=False,
    )
```

```python
import functools

import jax
import jax.numpy as jnp
from jax import lax
from jax.experimental import pallas as pl
from jax.experimental.pallas import tpu as pltpu
from jax.sharding import PartitionSpec as P

LOADING = 100.0
MESH = pl.DeviceIdType.MESH
F32 = jnp.float32
BF16 = jnp.bfloat16
CYC, DISH, CH, BEAM, PORT, TIME = 2, 9, 2, 36, 188, 128
SEC = 4
ROWS = CH * PORT
LANES = 384
TILES = LANES // TIME
WR = BEAM * CH
PER = WR // SEC
PARTS = 3
PART = DISH // PARTS
BLK = PART * PER
BLKP = 56
ALL = SEC * DISH
ALLP = 40


def dot(a, b):
    return lax.dot_general(a, b, (((1,), (0,)), ((), ())), preferred_element_type=F32)


def dot_t(a, b):
    return lax.dot_general(a, b, (((1,), (1,)), ((), ())), preferred_element_type=F32)


def iota(shape, dim):
    return lax.broadcasted_iota(jnp.int32, shape, dim)


def even_lanes(shape):
    return (iota(shape, 1) & 1) == 0


def split(x):
    high = x.astype(BF16)
    return high, (x - high.astype(F32)).astype(BF16)


def strided(ref, rows):
    return jnp.concatenate([ref[k, rows, :] for k in range(TILES)], axis=1)


def lane_up(x):
    return pltpu.roll(x, 1, 1)


def lane_down(x):
    return pltpu.roll(x, LANES - 1, 1)


def kernel(
    chans,
    volt, w_hbm, sat_hbm, offs_hbm, ang_hbm,
    wide, w_out,
    x, w_in, sat_in, offs, ang, we, sat_l, sat_r, steer, vv, pack, packed, halo_l, halo_r, ana, syn, nul, stage, sbuf, recv,
    in_sem, x_sem, sat_ssem, sat_rsem, halo_ssem, halo_rsem, beam_ssem, beam_rsem,
):
    me = lax.axis_index("chan")
    sec = lax.axis_index("section")
    left = lax.rem(me + chans - 1, chans)
    right = lax.rem(me + 1, chans)

    def load(c, d, z):
        return pltpu.make_async_copy(
            volt.at[c, z, d],
            x.at[c, z, d, pl.ds(0, ROWS)],
            x_sem.at[c, d, z],
        )

    def wait_voltages(c):
        for d in range(DISH):
            for z in range(2):
                load(c, d, z).wait()

    def voltage(c, d):
        return jnp.concatenate([x[c, 0, d], x[c, 1, d]], axis=1)

    sat_l[...] = jnp.zeros_like(sat_l)
    sat_r[...] = jnp.zeros_like(sat_r)
    halo_l[...] = jnp.zeros_like(halo_l)
    halo_r[...] = jnp.zeros_like(halo_r)

    barrier = pltpu.get_barrier_semaphore()
    for j in range(1, SEC):
        pl.semaphore_signal(
            barrier, inc=1, device_id={"section": lax.rem(sec + j, SEC)}, device_id_type=MESH
        )
    sides = ((me > 0, left), (me < chans - 1, right))
    for exists, peer in sides:

        @pl.when(exists)
        def _():
            pl.semaphore_signal(barrier, inc=1, device_id={"chan": peer}, device_id_type=MESH)

    small = [
        pltpu.make_async_copy(source, target, in_sem.at[i])
        for i, (source, target) in enumerate(
            ((ang_hbm, ang), (w_hbm, w_in), (sat_hbm, sat_in), (offs_hbm, offs))
        )
    ]
    for copy in small:
        copy.start()
    for c in range(CYC):
        for d in range(DISH):
            for z in range(2):
                load(c, d, z).start()

    def sat_copy(side):
        return pltpu.make_async_remote_copy(
            src_ref=sat_in,
            dst_ref=sat_r if side == 0 else sat_l,
            send_sem=sat_ssem.at[side],
            recv_sem=sat_rsem.at[side],
            device_id={"chan": left if side == 0 else right},
            device_id_type=MESH,
        )

    pl.semaphore_wait(barrier, SEC - 1 + sum(e.astype(jnp.int32) for e, _peer in sides))
    small[2].wait()
    for side in range(2):

        @pl.when(sides[side][0])
        def _():
            sat_copy(side).start()

    spread = (lax.shift_right_logical(iota((PORT, LANES), 1), 1) == iota((PORT, LANES), 0)).astype(
        F32
    ).astype(BF16)
    own = (iota((WR, LANES), 0) & 1) == (iota((WR, LANES), 1) & 1)
    for c in range(CYC):
        for d in range(DISH):
            for z in range(2):
                x[c, z, d, pl.ds(ROWS, LANES - ROWS), :] = jnp.zeros((LANES - ROWS, TIME), BF16)
    wide[:, pl.ds(ALL * PER, (ALLP - ALL) * PER), :] = jnp.zeros(
        (2 * CYC, (ALLP - ALL) * PER, TIME), F32
    )
    small[0].wait()
    grown_table = []
    for values in (jnp.cos(ang[...]), jnp.sin(ang[...])):
        for part in split(values):
            grown_table.append(dot(part, spread).astype(BF16))
    small[1].wait()
    for d in range(DISH):
        for z in range(2):
            grown = dot(w_in[z, d].reshape(WR, PORT), spread)
            we[d, pl.ds(z * WR, WR), :] = jnp.where(own, grown, 0.0).astype(BF16)

    def beams(c, k):
        dishes = range(PART * k, PART * (k + 1))
        if c == 1:
            project(dishes)
        for j, d in enumerate(dishes):
            both = dot(we[d], voltage(c, d))
            real = both[:WR, :TIME] + both[WR:, TIME:]
            imag = both[:WR, TIME:] - both[WR:, :TIME]
            for s in range(SEC):
                rows = pl.ds(j * PER, PER)
                stage[s, k, rows, pl.ds(0, TIME)] = real[s * PER : (s + 1) * PER]
                stage[s, k, rows, pl.ds(TIME, TIME)] = imag[s * PER : (s + 1) * PER]
        for s in range(SEC):
            sbuf[c, s, k] = stage[s, k].astype(BF16)

    def beam_copy(c, k, j):
        peer = lax.rem(sec + j, SEC)
        return pltpu.make_async_remote_copy(
            src_ref=sbuf.at[c, peer, k],
            dst_ref=recv.at[c, sec, k],
            send_sem=beam_ssem.at[c, k, j - 1],
            recv_sem=beam_rsem.at[c, k, j - 1],
            device_id={"section": peer},
            device_id_type=MESH,
        )

    def send_beams(c, k):
        for j in (2, 3, 1):
            beam_copy(c, k, j).start()
        recv[c, sec, k] = sbuf[c, sec, k]

    wait_voltages(0)
    for k in range(PARTS):
        beams(0, k)

    for side in range(2):

        @pl.when(sides[1 - side][0])
        def _():
            sat_copy(side).wait_recv()

    row = iota((8, TIME), 0)
    keep = (iota((8, LANES), 0) >= 4) == ((iota((8, LANES), 1) & 1) == 1)
    for c in range(CYC):
        own_s, left_s, right_s = (
            jnp.where((row & 1) == 0, ref[pl.ds(c, 1), pl.ds(0, 1)], ref[pl.ds(c, 1), pl.ds(1, 1)])
            for ref in (sat_in, sat_l, sat_r)
        )
        index = jnp.where((row & 3) < 2, own_s, jnp.where(row < 4, left_s, right_s))
        hot = (index == iota((8, TIME), 1)).astype(F32).astype(BF16)[:, :64]
        parts = [dot(hot, part) for part in grown_table]
        for i, (h, l) in enumerate(((0, 1), (2, 3))):
            steer[c, i] = parts[h] + parts[l]
        stacked = [jnp.where(keep, parts[i], 0.0) for i in (0, 2, 1, 3)]
        for i in range(4):
            ana[c, pl.ds(8 * i, 8), :] = stacked[i]

    even4 = even_lanes((4, LANES))

    def null_vectors(c):
        if c == 0:
            small[3].wait()
        times = (offs[pl.ds(c, 1), :] == iota((TIME, TIME), 0)).astype(F32).astype(BF16)
        count = dot_t(jnp.ones((8, TIME), BF16), times)
        probe = ana[c].astype(BF16)
        for first in range(0, DISH, 9):
            dishes = range(first, first + 9)
            outs = [dot(probe, voltage(c, d)) for d in dishes]
            lines = []
            for out in outs:
                out = out[:16] + out[16:]
                y_real = (out[:8, :TIME] + out[8:, TIME:]) * count
                y_imag = (out[8:, :TIME] - out[:8, TIME:]) * count
                pair = jnp.concatenate(
                    [
                        jnp.concatenate([y_real, -y_imag], axis=1),
                        jnp.concatenate([y_imag, y_real], axis=1),
                    ],
                    axis=0,
                )
                lines.append(jnp.concatenate(split(pair), axis=0))
            backs = []
            for j, d in enumerate(dishes):
                block = voltage(c, d)
                backs.append(dot_t(lines[j], block))
            for d, back in zip(dishes, backs):
                back = back[:16] + back[16:]
                for i in range(2):
                    kept = jnp.where(even4, back[8 * i : 8 * i + 4], back[8 * i + 4 : 8 * i + 8])
                    for k in range(TILES):
                        vv[c, k, pl.ds(8 * d + 4 * i, 4), :] = kept[:, k * TIME : (k + 1) * TIME]

    even = even_lanes((DISH, LANES))

    def halo_copy(c, side):
        return pltpu.make_async_remote_copy(
            src_ref=packed.at[c, side],
            dst_ref=(halo_r if side == 0 else halo_l).at[c],
            send_sem=halo_ssem.at[c, side],
            recv_sem=halo_rsem.at[c, side],
            device_id={"chan": left if side == 0 else right},
            device_id_type=MESH,
        )

    def take(c, q):
        return strided(vv.at[c], pl.ds(q, DISH, stride=8))

    def send_halo(c):
        for i in range(2):
            first, second = take(c, 4 * i + 2), take(c, 4 * i + 3)
            rows = pl.ds(i * DISH, DISH)
            pack[0, rows, :] = jnp.where(even, first, lane_up(second))
            pack[1, rows, :] = jnp.where(even, lane_down(first), second)
        packed[c] = pack[...]
        for side in range(2):

            @pl.when(sides[side][0])
            def _():
                halo_copy(c, side).start()

    pack[...] = jnp.zeros_like(pack)
    null_vectors(0)
    send_halo(0)
    wait_voltages(1)
    null_vectors(1)
    send_halo(1)
    for k in range(PARTS):
        send_beams(0, k)

    def lane_sum(v):
        e = jnp.sum(jnp.where(even, v, 0.0), axis=1, keepdims=True)
        o = jnp.sum(jnp.where(even, 0.0, v), axis=1, keepdims=True)
        return jnp.where(even, e, o)

    def project_vectors(c):
        for side in range(2):

            @pl.when(sides[1 - side][0])
            def _():
                halo_copy(c, side).wait_recv()

        u = []
        halos = [ref[c] for ref in (halo_l, halo_r)]
        for i in range(2):
            from_l, from_r = (h[i * DISH : (i + 1) * DISH] for h in halos)
            halo = (
                jnp.where(even, from_l, lane_up(from_r)),
                jnp.where(even, lane_down(from_l), from_r),
            )
            for s in range(2):
                v = take(c, 4 * i + s)
                v = v + jnp.where(even, lane_down(v), lane_up(v))
                u.append(v + halo[s] + LOADING * steer[c, i, pl.ds(s, 1), :])
        u0r, u1r, u0i, u1i = u
        inv0 = 1.0 / lane_sum(u0r * u0r + u0i * u0i)
        inv1 = 1.0 / lane_sum(u1r * u1r + u1i * u1i)
        t0r, t0i = u0r * inv0, u0i * inv0
        kr = lane_sum(t0r * u1r + t0i * u1i)
        ki = lane_sum(t0r * u1i - t0i * u1r)
        t1r = (u1r - (u0r * kr - u0i * ki)) * inv1
        t1i = (u1i - (u0r * ki + u0i * kr)) * inv1
        for q, (t, v) in enumerate(((t0r, u0r), (t0i, u0i), (t1r, u1r), (t1i, u1i))):
            for k in range(TILES):
                syn[k, pl.ds(16 * q, DISH), :] = t[:, k * TIME : (k + 1) * TIME]
                nul[k, pl.ds(16 * q, DISH), :] = v[:, k * TIME : (k + 1) * TIME]

    def project(dishes):
        inner, bases, changes = [], [], []
        for d in dishes:
            probe = jnp.concatenate(split(strided(syn, pl.ds(d, 4, stride=16))), axis=0)
            inner.append([dot_t(probe, we[d, pl.ds(z * WR, WR), :]) for z in range(2)])
        for d in dishes:
            high, low = split(strided(nul, pl.ds(d, 4, stride=16)))
            bases.append(jnp.concatenate([high, low, high], axis=0))
        for outs, basis in zip(inner, bases):
            gr, gi = (out[:4] + out[4:] for out in outs)
            first, second = [], []
            for s in range(2):
                cr = gr[2 * s : 2 * s + 1] + gi[2 * s + 1 : 2 * s + 2]
                ci = gi[2 * s : 2 * s + 1] - gr[2 * s + 1 : 2 * s + 2]
                first += [cr, -ci]
                second += [ci, cr]
            for rows in (first, second):
                c_high, c_low = split(jnp.concatenate(rows, axis=0))
                amount = jnp.concatenate([c_high, c_high, c_low], axis=0)
                changes.append(
                    lax.dot_general(
                        amount, basis, (((0,), (0,)), ((), ())), preferred_element_type=F32
                    )
                )
        for d in dishes:
            for z in range(2):
                new = we[d, pl.ds(z * WR, WR), :].astype(F32) - changes.pop(0)
                we[d, pl.ds(z * WR, WR), :] = jnp.where(own, new, 0.0).astype(BF16)

    project_vectors(0)
    for k in range(PARTS):
        beams(1, k)
        send_beams(1, k)

    project_vectors(1)
    gather = (lax.shift_right_logical(iota((LANES, PORT), 0), 1) == iota((LANES, PORT), 1)).astype(
        F32
    ).astype(BF16)
    for k in range(PARTS):
        project(range(PART * k, PART * (k + 1)))
    for d in range(DISH):
        for z in range(2):
            dense = dot(we[d, pl.ds(z * WR, WR), :], gather).astype(BF16)
            w_out[z, d] = dense.reshape(BEAM, CH, PORT)

    for c in range(CYC):
        for k in range(PARTS):
            for j in range(1, SEC):
                beam_copy(c, k, j).wait_recv()
            for s in range(SEC):
                block = recv[c, s, k].astype(F32)[:BLK]
                rows = pl.ds((s * PARTS + k) * BLK, BLK)
                for z in range(2):
                    wide[2 * c + z, rows, :] = block[:, z * TIME : (z + 1) * TIME]

    for c in range(CYC):
        for k in range(PARTS):
            for j in range(1, SEC):
                beam_copy(c, k, j).wait_send()
    for side in range(2):

        @pl.when(sides[side][0])
        def _():
            sat_copy(side).wait_send()
            for c in range(CYC):
                halo_copy(c, side).wait_send()


def correlate(wide, w_new, vis_hbm, w_hbm, vis, flat, corr, sems):
    weights = pltpu.make_async_copy(w_new, w_hbm, sems.at[0])
    weights.start()
    for r in range(PER):
        lanes = [wide[k, pl.ds(r, ALLP, stride=PER), :] for k in range(2 * CYC)]
        straight = jnp.concatenate(lanes, axis=1)
        turned = jnp.concatenate([lanes[1], -lanes[0], lanes[3], -lanes[2]], axis=1)
        right_side = straight.astype(BF16)
        result = dot_t(jnp.concatenate([straight, turned], axis=0).astype(BF16), right_side)
        result = result * (1.0 / (CYC * TIME))
        for z in range(2):
            corr[z, pl.ds(r * ALLP, ALLP), pl.ds(0, ALLP)] = result[z * ALLP : (z + 1) * ALLP]
    for z in range(2):
        for d in range(ALL):
            flat[z, :, pl.ds(d * ALL, ALL)] = corr[z, pl.ds(d, PER, stride=ALLP), :][:, :ALL]
        vis[z] = flat[z].reshape(DISH, CH, ALL * ALL)
        pltpu.make_async_copy(vis.at[z], vis_hbm.at[z], sems.at[1 + z]).start()
    weights.wait()
    for z in range(2):
        pltpu.make_async_copy(vis.at[z], vis_hbm.at[z], sems.at[1 + z]).wait()


def per_device(chans, voltages, weights, sat_index, offsets, angles):
    volt = voltages.transpose(0, 1, 2, 4, 3, 5).reshape(CYC, 2, DISH, ROWS, TIME)
    w_in = weights.transpose(0, 1, 3, 2, 4)
    sat = sat_index.reshape(CYC, 2)
    vmem = pl.BlockSpec(memory_space=pltpu.VMEM)
    hbm = pl.BlockSpec(memory_space=pltpu.HBM)
    dma = pltpu.SemaphoreType.DMA
    wide, new = pl.pallas_call(
        functools.partial(kernel, chans),
        out_shape=(
            jax.ShapeDtypeStruct((2 * CYC, ALLP * PER, TIME), F32),
            jax.ShapeDtypeStruct((2, DISH, BEAM, CH, PORT), BF16),
        ),
        in_specs=[hbm] * 5,
        out_specs=(vmem, vmem),
        scratch_shapes=[
            pltpu.VMEM((CYC, 2, DISH, LANES, TIME), BF16),
            pltpu.VMEM((2, DISH, BEAM, CH, PORT), BF16),
            pltpu.VMEM((CYC, 2), jnp.int32),
            pltpu.VMEM((CYC, TIME), jnp.int32),
            pltpu.VMEM((64, PORT), F32),
            pltpu.VMEM((DISH, 2 * WR, LANES), BF16),
            pltpu.VMEM((CYC, 2), jnp.int32),
            pltpu.VMEM((CYC, 2), jnp.int32),
            pltpu.VMEM((CYC, 2, 8, LANES), F32),
            pltpu.VMEM((CYC, TILES, DISH * 8, TIME), F32),
            pltpu.VMEM((2, 24, LANES), F32),
            pltpu.VMEM((CYC, 2, 24, LANES), F32),
            pltpu.VMEM((CYC, 24, LANES), F32),
            pltpu.VMEM((CYC, 24, LANES), F32),
            pltpu.VMEM((CYC, 32, LANES), F32),
            pltpu.VMEM((TILES, 64, TIME), F32),
            pltpu.VMEM((TILES, 64, TIME), F32),
            pltpu.VMEM((SEC, PARTS, BLKP, 2 * TIME), F32),
            pltpu.VMEM((CYC, SEC, PARTS, BLKP, 2 * TIME), BF16),
            pltpu.VMEM((CYC, SEC, PARTS, BLKP, 2 * TIME), BF16),
            dma((4,)),
            dma((CYC, DISH, 2)),
            dma((2,)),
            dma((2,)),
            dma((CYC, 2)),
            dma((CYC, 2)),
            dma((CYC, PARTS, SEC - 1)),
            dma((CYC, PARTS, SEC - 1)),
        ],
        compiler_params=pltpu.CompilerParams(
            collective_id=0, has_side_effects=True, vmem_limit_bytes=24 << 20
        ),
    )(*(pltpu.with_memory_space_constraint(a, pltpu.HBM) for a in (volt, w_in, sat, offsets, angles)))
    vis, new = pl.pallas_call(
        correlate,
        out_shape=(
            jax.ShapeDtypeStruct((2, DISH, CH, ALL * ALL), F32),
            jax.ShapeDtypeStruct((2, DISH, BEAM, CH, PORT), BF16),
        ),
        in_specs=[vmem, vmem],
        out_specs=(hbm, hbm),
        scratch_shapes=[
            pltpu.VMEM((2, DISH, CH, ALL * ALL), F32),
            pltpu.VMEM((2, PER, ALL * ALL), F32),
            pltpu.VMEM((2, PER * ALLP, TIME), F32),
            dma((3,)),
        ],
        compiler_params=pltpu.CompilerParams(vmem_limit_bytes=24 << 20),
    )(wide, new)
    return vis, new.transpose(0, 1, 3, 2, 4)


def solution(mesh):
    placed = (
        P(None, None, "section", "chan", None, None),
        P(None, "section", "chan", None, None),
        P(None, "chan", None),
        P(),
        P(),
    )
    return jax.shard_map(
        functools.partial(per_device, mesh.shape["chan"]),
        mesh=mesh,
        in_specs=placed,
        out_specs=(P(None, "section", "chan", None), P(None, "section", "chan", None, None)),
        check_vma=False,
    )
```

```python
import functools

import jax
import jax.numpy as jnp
from jax import lax
from jax.experimental import pallas as pl
from jax.experimental.pallas import tpu as pltpu
from jax.sharding import PartitionSpec as P

LOADING = 100.0
MESH = pl.DeviceIdType.MESH
F32 = jnp.float32
BF16 = jnp.bfloat16
CYC, DISH, CH, BEAM, PORT, TIME = 2, 9, 2, 36, 188, 128
SEC = 4
ROWS = CH * PORT
LANES = 384
TILES = LANES // TIME
WR = BEAM * CH
PER = WR // SEC
PARTS = 3
PART = DISH // PARTS
BLK = PART * PER
BLKP = 56
ALL = SEC * DISH
ALLP = 40


def dot(a, b):
    return lax.dot_general(a, b, (((1,), (0,)), ((), ())), preferred_element_type=F32)


def dot_t(a, b):
    return lax.dot_general(a, b, (((1,), (1,)), ((), ())), preferred_element_type=F32)


def iota(shape, dim):
    return lax.broadcasted_iota(jnp.int32, shape, dim)


def even_lanes(shape):
    return (iota(shape, 1) & 1) == 0


def split(x):
    high = x.astype(BF16)
    return high, (x - high.astype(F32)).astype(BF16)


def strided(ref, rows):
    return jnp.concatenate([ref[k, rows, :] for k in range(TILES)], axis=1)


def lane_up(x):
    return pltpu.roll(x, 1, 1)


def lane_down(x):
    return pltpu.roll(x, LANES - 1, 1)


def kernel(
    chans,
    volt, w_hbm, sat_hbm, offs_hbm, ang_hbm,
    wide, w_out,
    x, w_in, sat_in, offs, ang, we, sat_l, sat_r, steer, vv, pack, packed, halo_l, halo_r, ana, syn, nul, stage, sbuf, recv,
    in_sem, x_sem, sat_ssem, sat_rsem, halo_ssem, halo_rsem, beam_ssem, beam_rsem,
):
    me = lax.axis_index("chan")
    sec = lax.axis_index("section")
    left = lax.rem(me + chans - 1, chans)
    right = lax.rem(me + 1, chans)

    def load(c, d, z):
        return pltpu.make_async_copy(
            volt.at[c, z, d],
            x.at[c, z, d, pl.ds(0, ROWS)],
            x_sem.at[c, d, z],
        )

    def wait_voltages(c):
        for d in range(DISH):
            for z in range(2):
                load(c, d, z).wait()

    def voltage(c, d):
        return jnp.concatenate([x[c, 0, d], x[c, 1, d]], axis=1)

    sat_l[...] = jnp.zeros_like(sat_l)
    sat_r[...] = jnp.zeros_like(sat_r)
    halo_l[...] = jnp.zeros_like(halo_l)
    halo_r[...] = jnp.zeros_like(halo_r)

    barrier = pltpu.get_barrier_semaphore()
    for j in range(1, SEC):
        pl.semaphore_signal(
            barrier, inc=1, device_id={"section": lax.rem(sec + j, SEC)}, device_id_type=MESH
        )
    sides = ((me > 0, left), (me < chans - 1, right))
    for exists, peer in sides:

        @pl.when(exists)
        def _():
            pl.semaphore_signal(barrier, inc=1, device_id={"chan": peer}, device_id_type=MESH)

    small = [
        pltpu.make_async_copy(source, target, in_sem.at[i])
        for i, (source, target) in enumerate(
            ((ang_hbm, ang), (w_hbm, w_in), (sat_hbm, sat_in), (offs_hbm, offs))
        )
    ]
    for copy in small:
        copy.start()
    for c in range(CYC):
        for d in range(DISH):
            for z in range(2):
                load(c, d, z).start()

    def sat_copy(side):
        return pltpu.make_async_remote_copy(
            src_ref=sat_in,
            dst_ref=sat_r if side == 0 else sat_l,
            send_sem=sat_ssem.at[side],
            recv_sem=sat_rsem.at[side],
            device_id={"chan": left if side == 0 else right},
            device_id_type=MESH,
        )

    pl.semaphore_wait(barrier, SEC - 1 + sum(e.astype(jnp.int32) for e, _peer in sides))
    small[2].wait()
    for side in range(2):

        @pl.when(sides[side][0])
        def _():
            sat_copy(side).start()

    spread = (lax.shift_right_logical(iota((PORT, LANES), 1), 1) == iota((PORT, LANES), 0)).astype(
        F32
    ).astype(BF16)
    own = (iota((WR, LANES), 0) & 1) == (iota((WR, LANES), 1) & 1)
    for c in range(CYC):
        for d in range(DISH):
            for z in range(2):
                x[c, z, d, pl.ds(ROWS, LANES - ROWS), :] = jnp.zeros((LANES - ROWS, TIME), BF16)
    wide[:, pl.ds(ALL * PER, (ALLP - ALL) * PER), :] = jnp.zeros(
        (2 * CYC, (ALLP - ALL) * PER, TIME), F32
    )
    small[0].wait()
    grown_table = []
    for values in (jnp.cos(ang[...]), jnp.sin(ang[...])):
        for part in split(values):
            grown_table.append(dot(part, spread).astype(BF16))
    small[1].wait()
    for d in range(DISH):
        for z in range(2):
            grown = dot(w_in[z, d].reshape(WR, PORT), spread)
            we[d, pl.ds(z * WR, WR), :] = jnp.where(own, grown, 0.0).astype(BF16)

    def beams(c, k):
        dishes = range(PART * k, PART * (k + 1))
        if c == 1:
            project(dishes)
        for j, d in enumerate(dishes):
            both = dot(we[d], voltage(c, d))
            real = both[:WR, :TIME] + both[WR:, TIME:]
            imag = both[:WR, TIME:] - both[WR:, :TIME]
            for s in range(SEC):
                rows = pl.ds(j * PER, PER)
                stage[s, k, rows, pl.ds(0, TIME)] = real[s * PER : (s + 1) * PER]
                stage[s, k, rows, pl.ds(TIME, TIME)] = imag[s * PER : (s + 1) * PER]
        for s in range(SEC):
            sbuf[c, s, k] = stage[s, k].astype(BF16)

    def beam_copy(c, k, j):
        peer = lax.rem(sec + j, SEC)
        return pltpu.make_async_remote_copy(
            src_ref=sbuf.at[c, peer, k],
            dst_ref=recv.at[c, sec, k],
            send_sem=beam_ssem.at[c, k, j - 1],
            recv_sem=beam_rsem.at[c, k, j - 1],
            device_id={"section": peer},
            device_id_type=MESH,
        )

    def send_beams(c, k):
        for j in (2, 3, 1):
            beam_copy(c, k, j).start()
        recv[c, sec, k] = sbuf[c, sec, k]

    wait_voltages(0)
    for k in range(PARTS):
        beams(0, k)
        send_beams(0, k)

    for side in range(2):

        @pl.when(sides[1 - side][0])
        def _():
            sat_copy(side).wait_recv()

    row = iota((8, TIME), 0)
    keep = (iota((8, LANES), 0) >= 4) == ((iota((8, LANES), 1) & 1) == 1)
    for c in range(CYC):
        own_s, left_s, right_s = (
            jnp.where((row & 1) == 0, ref[pl.ds(c, 1), pl.ds(0, 1)], ref[pl.ds(c, 1), pl.ds(1, 1)])
            for ref in (sat_in, sat_l, sat_r)
        )
        index = jnp.where((row & 3) < 2, own_s, jnp.where(row < 4, left_s, right_s))
        hot = (index == iota((8, TIME), 1)).astype(F32).astype(BF16)[:, :64]
        parts = [dot(hot, part) for part in grown_table]
        for i, (h, l) in enumerate(((0, 1), (2, 3))):
            steer[c, i] = parts[h] + parts[l]
        stacked = [jnp.where(keep, parts[i], 0.0) for i in (0, 2, 1, 3)]
        for i in range(4):
            ana[c, pl.ds(8 * i, 8), :] = stacked[i]

    even4 = even_lanes((4, LANES))

    def null_vectors(c):
        if c == 0:
            small[3].wait()
        times = (offs[pl.ds(c, 1), :] == iota((TIME, TIME), 0)).astype(F32).astype(BF16)
        count = dot_t(jnp.ones((8, TIME), BF16), times)
        probe = ana[c].astype(BF16)
        for first in range(0, DISH, 9):
            dishes = range(first, first + 9)
            outs = [dot(probe, voltage(c, d)) for d in dishes]
            lines = []
            for out in outs:
                out = out[:16] + out[16:]
                y_real = (out[:8, :TIME] + out[8:, TIME:]) * count
                y_imag = (out[8:, :TIME] - out[:8, TIME:]) * count
                pair = jnp.concatenate(
                    [
                        jnp.concatenate([y_real, -y_imag], axis=1),
                        jnp.concatenate([y_imag, y_real], axis=1),
                    ],
                    axis=0,
                )
                lines.append(jnp.concatenate(split(pair), axis=0))
            backs = []
            for j, d in enumerate(dishes):
                block = voltage(c, d)
                backs.append(dot_t(lines[j], block))
            for d, back in zip(dishes, backs):
                back = back[:16] + back[16:]
                for i in range(2):
                    kept = jnp.where(even4, back[8 * i : 8 * i + 4], back[8 * i + 4 : 8 * i + 8])
                    for k in range(TILES):
                        vv[c, k, pl.ds(8 * d + 4 * i, 4), :] = kept[:, k * TIME : (k + 1) * TIME]

    even = even_lanes((DISH, LANES))

    def halo_copy(c, side):
        return pltpu.make_async_remote_copy(
            src_ref=packed.at[c, side],
            dst_ref=(halo_r if side == 0 else halo_l).at[c],
            send_sem=halo_ssem.at[c, side],
            recv_sem=halo_rsem.at[c, side],
            device_id={"chan": left if side == 0 else right},
            device_id_type=MESH,
        )

    def take(c, q):
        return strided(vv.at[c], pl.ds(q, DISH, stride=8))

    def send_halo(c):
        for i in range(2):
            first, second = take(c, 4 * i + 2), take(c, 4 * i + 3)
            rows = pl.ds(i * DISH, DISH)
            pack[0, rows, :] = jnp.where(even, first, lane_up(second))
            pack[1, rows, :] = jnp.where(even, lane_down(first), second)
        packed[c] = pack[...]
        for side in range(2):

            @pl.when(sides[side][0])
            def _():
                halo_copy(c, side).start()

    pack[...] = jnp.zeros_like(pack)
    null_vectors(0)
    send_halo(0)
    wait_voltages(1)
    null_vectors(1)
    send_halo(1)

    def lane_sum(v):
        e = jnp.sum(jnp.where(even, v, 0.0), axis=1, keepdims=True)
        o = jnp.sum(jnp.where(even, 0.0, v), axis=1, keepdims=True)
        return jnp.where(even, e, o)

    def project_vectors(c):
        for side in range(2):

            @pl.when(sides[1 - side][0])
            def _():
                halo_copy(c, side).wait_recv()

        u = []
        halos = [ref[c] for ref in (halo_l, halo_r)]
        for i in range(2):
            from_l, from_r = (h[i * DISH : (i + 1) * DISH] for h in halos)
            halo = (
                jnp.where(even, from_l, lane_up(from_r)),
                jnp.where(even, lane_down(from_l), from_r),
            )
            for s in range(2):
                v = take(c, 4 * i + s)
                v = v + jnp.where(even, lane_down(v), lane_up(v))
                u.append(v + halo[s] + LOADING * steer[c, i, pl.ds(s, 1), :])
        u0r, u1r, u0i, u1i = u
        inv0 = 1.0 / lane_sum(u0r * u0r + u0i * u0i)
        inv1 = 1.0 / lane_sum(u1r * u1r + u1i * u1i)
        t0r, t0i = u0r * inv0, u0i * inv0
        kr = lane_sum(t0r * u1r + t0i * u1i)
        ki = lane_sum(t0r * u1i - t0i * u1r)
        t1r = (u1r - (u0r * kr - u0i * ki)) * inv1
        t1i = (u1i - (u0r * ki + u0i * kr)) * inv1
        for q, (t, v) in enumerate(((t0r, u0r), (t0i, u0i), (t1r, u1r), (t1i, u1i))):
            for k in range(TILES):
                syn[k, pl.ds(16 * q, DISH), :] = t[:, k * TIME : (k + 1) * TIME]
                nul[k, pl.ds(16 * q, DISH), :] = v[:, k * TIME : (k + 1) * TIME]

    def project(dishes):
        inner, bases, changes = [], [], []
        for d in dishes:
            probe = jnp.concatenate(split(strided(syn, pl.ds(d, 4, stride=16))), axis=0)
            inner.append([dot_t(probe, we[d, pl.ds(z * WR, WR), :]) for z in range(2)])
        for d in dishes:
            high, low = split(strided(nul, pl.ds(d, 4, stride=16)))
            bases.append(jnp.concatenate([high, low, high], axis=0))
        for outs, basis in zip(inner, bases):
            gr, gi = (out[:4] + out[4:] for out in outs)
            first, second = [], []
            for s in range(2):
                cr = gr[2 * s : 2 * s + 1] + gi[2 * s + 1 : 2 * s + 2]
                ci = gi[2 * s : 2 * s + 1] - gr[2 * s + 1 : 2 * s + 2]
                first += [cr, -ci]
                second += [ci, cr]
            for rows in (first, second):
                c_high, c_low = split(jnp.concatenate(rows, axis=0))
                amount = jnp.concatenate([c_high, c_high, c_low], axis=0)
                changes.append(
                    lax.dot_general(
                        amount, basis, (((0,), (0,)), ((), ())), preferred_element_type=F32
                    )
                )
        for d in dishes:
            for z in range(2):
                new = we[d, pl.ds(z * WR, WR), :].astype(F32) - changes.pop(0)
                we[d, pl.ds(z * WR, WR), :] = jnp.where(own, new, 0.0).astype(BF16)

    project_vectors(0)
    for k in range(PARTS):
        beams(1, k)
        send_beams(1, k)

    project_vectors(1)
    gather = (lax.shift_right_logical(iota((LANES, PORT), 0), 1) == iota((LANES, PORT), 1)).astype(
        F32
    ).astype(BF16)
    for k in range(PARTS):
        project(range(PART * k, PART * (k + 1)))
    for d in range(DISH):
        dense = dot(we[d], gather)
        for z in range(2):
            part = dense[z * WR : (z + 1) * WR].astype(BF16)
            w_out[z, d] = part.reshape(BEAM, CH, PORT)

    for c in range(CYC):
        for k in range(PARTS):
            for j in range(1, SEC):
                beam_copy(c, k, j).wait_recv()
            for s in range(SEC):
                block = recv[c, s, k].astype(F32)[:BLK]
                rows = pl.ds((s * PARTS + k) * BLK, BLK)
                for z in range(2):
                    wide[2 * c + z, rows, :] = block[:, z * TIME : (z + 1) * TIME]

    for c in range(CYC):
        for k in range(PARTS):
            for j in range(1, SEC):
                beam_copy(c, k, j).wait_send()
    for side in range(2):

        @pl.when(sides[side][0])
        def _():
            sat_copy(side).wait_send()
            for c in range(CYC):
                halo_copy(c, side).wait_send()


def correlate(wide, w_new, vis_hbm, w_hbm, vis, flat, corr, sems):
    weights = pltpu.make_async_copy(w_new, w_hbm, sems.at[0])
    weights.start()
    for r in range(PER):
        lanes = [wide[k, pl.ds(r, ALLP, stride=PER), :] for k in range(2 * CYC)]
        straight = jnp.concatenate(lanes, axis=1)
        turned = jnp.concatenate([lanes[1], -lanes[0], lanes[3], -lanes[2]], axis=1)
        right_side = straight.astype(BF16)
        result = dot_t(jnp.concatenate([straight, turned], axis=0).astype(BF16), right_side)
        result = result * (1.0 / (CYC * TIME))
        for z in range(2):
            corr[z, pl.ds(r * ALLP, ALLP), pl.ds(0, ALLP)] = result[z * ALLP : (z + 1) * ALLP]
    for z in range(2):
        for d in range(ALL):
            flat[z, :, pl.ds(d * ALL, ALL)] = corr[z, pl.ds(d, PER, stride=ALLP), :][:, :ALL]
        vis[z] = flat[z].reshape(DISH, CH, ALL * ALL)
        pltpu.make_async_copy(vis.at[z], vis_hbm.at[z], sems.at[1 + z]).start()
    weights.wait()
    for z in range(2):
        pltpu.make_async_copy(vis.at[z], vis_hbm.at[z], sems.at[1 + z]).wait()


def per_device(chans, voltages, weights, sat_index, offsets, angles):
    volt = voltages.transpose(0, 1, 2, 4, 3, 5).reshape(CYC, 2, DISH, ROWS, TIME)
    w_in = weights.transpose(0, 1, 3, 2, 4)
    sat = sat_index.reshape(CYC, 2)
    vmem = pl.BlockSpec(memory_space=pltpu.VMEM)
    hbm = pl.BlockSpec(memory_space=pltpu.HBM)
    dma = pltpu.SemaphoreType.DMA
    wide, new = pl.pallas_call(
        functools.partial(kernel, chans),
        out_shape=(
            jax.ShapeDtypeStruct((2 * CYC, ALLP * PER, TIME), F32),
            jax.ShapeDtypeStruct((2, DISH, BEAM, CH, PORT), BF16),
        ),
        in_specs=[hbm] * 5,
        out_specs=(vmem, vmem),
        scratch_shapes=[
            pltpu.VMEM((CYC, 2, DISH, LANES, TIME), BF16),
            pltpu.VMEM((2, DISH, BEAM, CH, PORT), BF16),
            pltpu.VMEM((CYC, 2), jnp.int32),
            pltpu.VMEM((CYC, TIME), jnp.int32),
            pltpu.VMEM((64, PORT), F32),
            pltpu.VMEM((DISH, 2 * WR, LANES), BF16),
            pltpu.VMEM((CYC, 2), jnp.int32),
            pltpu.VMEM((CYC, 2), jnp.int32),
            pltpu.VMEM((CYC, 2, 8, LANES), F32),
            pltpu.VMEM((CYC, TILES, DISH * 8, TIME), F32),
            pltpu.VMEM((2, 24, LANES), F32),
            pltpu.VMEM((CYC, 2, 24, LANES), F32),
            pltpu.VMEM((CYC, 24, LANES), F32),
            pltpu.VMEM((CYC, 24, LANES), F32),
            pltpu.VMEM((CYC, 32, LANES), F32),
            pltpu.VMEM((TILES, 64, TIME), F32),
            pltpu.VMEM((TILES, 64, TIME), F32),
            pltpu.VMEM((SEC, PARTS, BLKP, 2 * TIME), F32),
            pltpu.VMEM((CYC, SEC, PARTS, BLKP, 2 * TIME), BF16),
            pltpu.VMEM((CYC, SEC, PARTS, BLKP, 2 * TIME), BF16),
            dma((4,)),
            dma((CYC, DISH, 2)),
            dma((2,)),
            dma((2,)),
            dma((CYC, 2)),
            dma((CYC, 2)),
            dma((CYC, PARTS, SEC - 1)),
            dma((CYC, PARTS, SEC - 1)),
        ],
        compiler_params=pltpu.CompilerParams(
            collective_id=0, has_side_effects=True, vmem_limit_bytes=24 << 20
        ),
    )(*(pltpu.with_memory_space_constraint(a, pltpu.HBM) for a in (volt, w_in, sat, offsets, angles)))
    vis, new = pl.pallas_call(
        correlate,
        out_shape=(
            jax.ShapeDtypeStruct((2, DISH, CH, ALL * ALL), F32),
            jax.ShapeDtypeStruct((2, DISH, BEAM, CH, PORT), BF16),
        ),
        in_specs=[vmem, vmem],
        out_specs=(hbm, hbm),
        scratch_shapes=[
            pltpu.VMEM((2, DISH, CH, ALL * ALL), F32),
            pltpu.VMEM((2, PER, ALL * ALL), F32),
            pltpu.VMEM((2, PER * ALLP, TIME), F32),
            dma((3,)),
        ],
        compiler_params=pltpu.CompilerParams(vmem_limit_bytes=24 << 20),
    )(wide, new)
    return vis, new.transpose(0, 1, 3, 2, 4)


def solution(mesh):
    placed = (
        P(None, None, "section", "chan", None, None),
        P(None, "section", "chan", None, None),
        P(None, "chan", None),
        P(),
        P(),
    )
    return jax.shard_map(
        functools.partial(per_device, mesh.shape["chan"]),
        mesh=mesh,
        in_specs=placed,
        out_specs=(P(None, "section", "chan", None), P(None, "section", "chan", None, None)),
        check_vma=False,
    )
```
